256 devices in a mesh: grp: 128 (over z, x, y), rep: 2 (over core).
Axes of the slice: x: 4, y: 4, z: 8, core: 2. Of those that a mesh axis runs over, the one named last changes fastest.
Arguments:
- vectors: bfloat16 [32768, 768], P(('grp', 'rep')), may hold values from -6 to 6
- list_ids: int32 [32768, 8], P(('grp', 'rep')), may hold values from -1 to 65535, as said below
- spill_weight: int32 [32768, 8], P(('grp', 'rep')), may hold values from 1 to 4
- list_pos: int32 [65536], replicated, may hold values from 0 to 65535, as said below
- old_centroids: float32 [65536, 768], P('grp'), may hold values from -12 to 12
Outputs:
- refined: float32 [65536, 768], P('grp')
- new_dist: float32 [32768, 8], P(('grp', 'rep'))
The draws below stay inside these ranges and needn't reach their ends.
Inputs may be any that keep to these rules, and one draw needn't show every extreme that they name: `list_ids`: entries are list numbers or -1; the lists of one row are distinct. List l is owned by grp index list_pos[l] // 512. Among the rows of one device (aligned blocks of 128 rows), at most 4 slots name lists of one owner, and in every block some owner gets exactly 4. `list_pos`: A permutation of the list numbers.
All inputs are finite; a program needn't handle non-finite values.
Results may differ from the reference program's by a relative error of at most 0.0003.
Values may be sent and summed in bfloat16 or wider, within the bound.
No kernel may reach another device: no remote copies, remote signals or barrier semaphores. Data moves between devices by JAX's collectives and lax.ppermute only.
A program may use at most 64 MiB of HBM per device.

```python
import jax
import jax.numpy as jnp
from jax import lax

D = 768
K = 8
V_DEV = 128
LPO = 512
OWNERS = 128
VECS = 32768
LISTS = 65536
CAP = 4


def lists_layout(key):
    list_pos = jax.random.permutation(jax.random.fold_in(key, 11), LISTS).astype(jnp.int32)
    at_position = jnp.argsort(list_pos, stable=True).astype(jnp.int32)
    hot_owner = jax.random.randint(jax.random.fold_in(key, 12), (OWNERS,), 0, 8) == 0
    block_count = VECS // V_DEV
    block_keys = jax.random.split(jax.random.fold_in(key, 13), block_count)

    def one_block(block_key):
        key_one, key_two, key_three, key_four = jax.random.split(block_key, 4)
        counts = jnp.where(hot_owner, CAP, jax.random.randint(key_one, (OWNERS,), CAP // 4, CAP // 2 + 1))
        full_owner = jax.random.randint(key_two, (), 0, OWNERS)
        counts = jnp.where(jnp.arange(OWNERS) == full_owner, CAP, counts)
        owner_of = jnp.repeat(jnp.arange(OWNERS, dtype=jnp.int32), CAP)
        seat_number = jnp.tile(jnp.arange(CAP, dtype=jnp.int32), OWNERS)
        tickets = jnp.where(seat_number < counts[owner_of], owner_of, -1).astype(jnp.int32)
        padding = jnp.full((V_DEV * K - OWNERS * CAP,), -1, jnp.int32)
        tickets = jnp.concatenate([tickets, padding])
        tickets = jax.random.permutation(key_three, tickets).reshape(V_DEV, K)
        column = jnp.arange(K, dtype=jnp.int32)[None, :]
        local_row = column + K * jax.random.randint(key_four, (V_DEV, K), 0, LPO // K)
        position = jnp.maximum(tickets, 0) * LPO + local_row
        return jnp.where(tickets >= 0, at_position[position], -1).astype(jnp.int32)
    list_ids = jax.vmap(one_block)(block_keys).reshape(VECS, K)
    return (list_pos, list_ids)


def draw_list_ids(key, part):
    return lists_layout(key)[1]


def draw_list_pos(key, part):
    return lists_layout(key)[0]


def touch_ends(result, own_key, smallest, top_value):
    index_at = [jax.random.randint(jax.random.fold_in(own_key, axis), (), 0, length) for axis, length in enumerate(result.shape)]
    longest = result.shape.index(max(result.shape))
    next_to = index_at[:longest] + [(index_at[longest] + 1) % result.shape[longest]] + index_at[longest + 1:]
    return result.at[tuple(index_at)].set(smallest).at[tuple(next_to)].set(top_value)


def level_of(own_key, shape, cuts, least, top_value):
    factor_of, own = 1.0, jax.random.fold_in(own_key, 6)
    for dim, parts in cuts:
        draws = jnp.exp(jax.random.uniform(jax.random.fold_in(own, dim), (parts,), jnp.float32, least / len(cuts), top_value / len(cuts)))
        factor_of = factor_of * jnp.repeat(draws, shape[dim] // parts).reshape([-1 if axis == dim else 1 for axis in range(len(shape))])
    return factor_of


def normal_values(key, dims, deviation, bound, shards=(), held_as=jnp.bfloat16):
    array = deviation * jax.random.normal(key, dims, jnp.float32)
    if shards:
        array = array * level_of(key, dims, shards, -0.22, 0.18)
    return jnp.clip(array, -bound, bound).astype(held_as)


def setup_inputs(seed: int = 0) -> dict:
    keys = jax.random.split(jax.random.key(seed), 6)
    vectors = normal_values(keys[0], (VECS, D), 1.0, 6.0, ((0, 256),))
    list_ids = draw_list_ids(jax.random.fold_in(keys[5], 71), 0)
    spill_weight = touch_ends(jax.random.randint(keys[2], (VECS, K), 1, 5), jax.random.fold_in(keys[2], 1), 1, 4).astype(jnp.int32)
    list_pos = draw_list_pos(jax.random.fold_in(keys[5], 71), 0)
    old_centroids = normal_values(keys[4], (LISTS, D), 2.0, 12.0, ((0, 128),), jnp.float32)
    return dict(vectors=vectors, list_ids=list_ids, spill_weight=spill_weight, list_pos=list_pos, old_centroids=old_centroids)


def reference(vectors, list_ids, spill_weight, list_pos, old_centroids):
    block_count = VECS // V_DEV
    is_live = list_ids >= 0
    places = jnp.where(is_live, list_pos[jnp.maximum(list_ids, 0)], 0).astype(jnp.int32)
    weights = jnp.where(is_live, spill_weight.astype(jnp.float32), jnp.float32(0.0))
    vector_blocks = vectors.reshape(block_count, V_DEV, D)
    place_blocks = places.reshape(block_count, V_DEV, K)
    weight_blocks = weights.reshape(block_count, V_DEV, K)

    def accumulate(running, piece_item):
        weighted_sums, totals = running
        rows_in, place_in, weight_in = piece_item
        row_values = rows_in.astype(jnp.float32)
        centre_rows = old_centroids[place_in]
        sq_norms = jnp.sum((row_values[:, None, :] - centre_rows) ** 2, axis=-1)
        shares = weight_in / (1.0 + sq_norms / D)
        flat_places = place_in.reshape(-1)
        weighted_sums = weighted_sums.at[flat_places].add((shares[:, :, None] * row_values[:, None, :]).reshape(-1, D))
        totals = totals.at[flat_places].add(shares.reshape(-1))
        return (weighted_sums, totals), jnp.float32(0.0)

    start_state = (jnp.zeros((LISTS, D), jnp.float32), jnp.zeros((LISTS,), jnp.float32))
    final_state, unused = lax.scan(accumulate, start_state, (vector_blocks, place_blocks, weight_blocks))
    weighted_sums, totals = final_state
    refined = (old_centroids + weighted_sums) / (1.0 + totals[:, None])

    def distance(piece_item):
        rows_in, place_in = piece_item
        row_values = rows_in.astype(jnp.float32)
        return jnp.sum((row_values[:, None, :] - refined[place_in]) ** 2, axis=-1) / D

    spread = lax.map(distance, (vector_blocks, place_blocks)).reshape(VECS, K)
    new_dist = jnp.where(is_live, spread, jnp.float32(0.0))
    return refined, new_dist
```

```python
import jax
import jax.numpy as jnp
from jax import lax
from jax.experimental import pallas as pl
from jax.experimental.pallas import tpu as pltpu
from jax.sharding import PartitionSpec as P

LANES = 128
VMEM_LIMIT = 24 * 2**20
F32 = jnp.float32
BF16 = jnp.bfloat16


def iota(shape, dim):
    return lax.broadcasted_iota(jnp.int32, shape, dim)


def ones_where(mask):
    return jnp.where(mask, F32(1), F32(0)).astype(BF16)


def dot(a, b, contract=(1, 0)):
    return lax.dot_general(
        a, b, (((contract[0],), (contract[1],)), ((), ())), preferred_element_type=F32
    )


def pieces(value, count):
    result = []
    for _ in range(count):
        part = value.astype(BF16)
        result.append(part)
        value = value - part.astype(F32)
    return result


def route_kernel(ids_ref, weight_ref, table_ref, vectors_ref, send_ref, seat_ref, *, cap, lists_here):
    slots, rows = ids_ref.shape
    seats, width = send_ref.shape
    owners = seats // cap
    feature_dim = vectors_ref.shape[1]
    table = table_ref[...]
    digits = jnp.concatenate(
        [(table >> 8).astype(F32).astype(BF16), (table & 255).astype(F32).astype(BF16)], axis=1
    )
    ids = ids_ref[...]
    live = ids >= 0
    safe = jnp.maximum(ids, 0)
    high, low = safe >> 7, safe & 127
    row_of_table = iota((table.shape[0], rows), 0)
    picks = jnp.concatenate(
        [ones_where(row_of_table == high[k : k + 1]) for k in range(slots)], axis=1
    )
    found = dot(digits, picks, (0, 0))
    found = found[:LANES] * 256 + found[LANES:]
    lane_of_table = iota((LANES, rows), 0)
    place = jnp.concatenate(
        [
            jnp.sum(
                jnp.where(lane_of_table == low[k : k + 1], found[:, k * rows : (k + 1) * rows], 0.0),
                axis=0,
                keepdims=True,
            )
            for k in range(slots)
        ],
        axis=0,
    ).astype(jnp.int32)
    owner = jnp.where(live, place // lists_here, owners)
    code = (place % lists_here) * 8 + weight_ref[...]

    owner_iota = iota((owners, rows), 0)
    at_owner = [owner_iota == owner[k : k + 1] for k in range(slots)]
    before = ones_where(iota((rows, 2 * rows), 0) < iota((rows, 2 * rows), 1))
    counted = dot(jnp.concatenate([ones_where(m) for m in at_owner], axis=0), before)
    carried = jnp.zeros((owners, rows), F32)
    ranks = []
    for k in range(slots):
        here = counted[k * owners : (k + 1) * owners]
        rank = jnp.where(at_owner[k], here[:, :rows] + carried, 0.0)
        ranks.append(jnp.sum(rank, axis=0, keepdims=True))
        carried = carried + here[:, rows:]
    rank = jnp.concatenate(ranks, axis=0).astype(jnp.int32)
    seat = jnp.where(live, owner * cap + rank, -1)
    seat_ref[...] = seat

    seat_iota = iota((seats, rows), 0)
    taken = jnp.zeros((seats, rows), F32)
    codes = jnp.zeros((seats, rows), jnp.int32)
    for k in range(slots):
        match = seat_iota == seat[k : k + 1]
        taken = jnp.where(match, 1.0, taken)
        codes = jnp.where(match, code[k : k + 1], codes)
    taken = taken.astype(BF16)
    send_ref[:, :feature_dim] = dot(taken, vectors_ref[...]).astype(BF16)
    meta = jnp.concatenate(
        [(codes >> 6).astype(F32).astype(BF16), (codes & 63).astype(F32).astype(BF16), taken], axis=1
    )
    columns = (width - feature_dim)
    spread = ones_where(iota((3 * rows, columns), 0) // rows == iota((3 * rows, columns), 1))
    send_ref[:, feature_dim:] = dot(meta, spread).astype(BF16)


def seats_of(got_ref, lists_here, feature_dim):
    meta = got_ref[:, feature_dim:].astype(F32)
    code = (meta[:, 0:1] * 64 + meta[:, 1:2]).astype(jnp.int32)
    weight = (code & 7).astype(F32)
    chosen = ones_where(iota((got_ref.shape[0], lists_here), 1) == (code >> 3))
    return chosen, weight


def sums_of(got_ref, centroids):
    lists_here, feature_dim = centroids.shape
    chosen, weight = seats_of(got_ref, lists_here, feature_dim)
    centre = sum(dot(chosen, part) for part in pieces(centroids, 2))
    values = got_ref[...].astype(F32)
    sq_norms = jnp.sum((values[:, :feature_dim] - centre) ** 2, axis=1, keepdims=True)
    shares = weight / (1.0 + sq_norms / feature_dim)
    return sum(dot(chosen, part, (0, 0)) for part in pieces(values * shares, 2))


def own_sums_kernel(got_ref, centroids_ref, sums_ref):
    sums_ref[...] = sums_of(got_ref, centroids_ref[...])


def refine_kernel(own_sums_ref, peer_ref, got_ref, centroids_ref, refined_ref, dist_ref, *, cap):
    centroids = centroids_ref[...]
    lists_here, feature_dim = centroids.shape
    sums = own_sums_ref[...] + sums_of(peer_ref, centroids)
    totals = sums[:, feature_dim + 2 : feature_dim + 3]
    refined = (centroids + sums[:, :feature_dim]) / (1.0 + totals)
    refined_ref[...] = refined
    chosen, _ = seats_of(got_ref, lists_here, feature_dim)
    centre = sum(dot(chosen, part) for part in pieces(refined, 2))
    values = got_ref[:, :feature_dim].astype(F32)
    dist = jnp.sum((values - centre) ** 2, axis=1, keepdims=True) / feature_dim
    seats = got_ref.shape[0]
    owners = seats // cap
    spread = jnp.where(iota((seats, LANES), 0) % cap == iota((seats, LANES), 1), dist, 0.0)
    gather = ones_where(iota((owners, seats), 1) // cap == iota((owners, seats), 0))
    dist_ref[...] = sum(dot(gather, part) for part in pieces(spread, 3))


def pick_kernel(dist_ref, seat_ref, out_ref, *, cap):
    slots, rows = seat_ref.shape
    owners = dist_ref.shape[0]
    seat = seat_ref[...]
    by_rank = dist_ref[...].T[:8]
    owner_iota = iota((owners, rows), 0)
    at_owner = jnp.concatenate(
        [ones_where(owner_iota == (seat[k : k + 1] // cap)) for k in range(slots)], axis=1
    )
    found = sum(dot(part, at_owner) for part in pieces(by_rank, 3))
    rank_iota = iota((8, rows), 0)
    picked = jnp.concatenate(
        [
            jnp.sum(
                jnp.where(
                    rank_iota == seat[k : k + 1] % cap, found[:, k * rows : (k + 1) * rows], 0.0
                ),
                axis=0,
                keepdims=True,
            )
            for k in range(slots)
        ],
        axis=0,
    )
    out_ref[...] = jnp.where(seat >= 0, picked, 0.0)


def on_chip(kernel, outs, *args, name):
    whole = pl.BlockSpec(memory_space=pltpu.VMEM)
    return pl.pallas_call(
        kernel,
        out_shape=outs,
        in_specs=[whole] * len(args),
        out_specs=jax.tree.map(lambda _: whole, outs),
        compiler_params=pltpu.CompilerParams(vmem_limit_bytes=VMEM_LIMIT),
        name=name,
    )(*args)


def shards(vectors, list_ids, spill_weight, list_pos, old_centroids):
    owners = lax.axis_size("grp")
    row_count, slot_count = list_ids.shape
    lists_here, feature_dim = old_centroids.shape
    cap = row_count * slot_count // (2 * owners)
    seats = owners * cap
    width = feature_dim + LANES
    struct = jax.ShapeDtypeStruct

    send, seat = on_chip(
        lambda *refs: route_kernel(*refs, cap=cap, lists_here=lists_here),
        (struct((seats, width), BF16), struct((slot_count, row_count), jnp.int32)),
        list_ids.T,
        spill_weight.T,
        list_pos.reshape(-1, LANES),
        vectors,
        name="route",
    )
    got = lax.all_to_all(send.reshape(owners, cap, width), "grp", 0, 0, tiled=True)
    got = got.reshape(seats, width)
    peer = lax.ppermute(got, "rep", [(0, 1), (1, 0)])
    own_sums = on_chip(
        own_sums_kernel, struct((lists_here, width), F32), got, old_centroids, name="own_sums"
    )
    refined, owner_dist = on_chip(
        lambda *refs: refine_kernel(*refs, cap=cap),
        (struct((lists_here, feature_dim), F32), struct((owners, LANES), F32)),
        own_sums,
        peer,
        got,
        old_centroids,
        name="refine",
    )
    seat_dist = lax.all_to_all(owner_dist.reshape(owners, 1, LANES), "grp", 0, 0, tiled=True)
    new_dist = on_chip(
        lambda *refs: pick_kernel(*refs, cap=cap),
        struct((slot_count, row_count), F32),
        seat_dist.reshape(owners, LANES),
        seat,
        name="pick",
    )
    return refined, new_dist.T


def solution(mesh):
    return jax.shard_map(
        shards,
        mesh=mesh,
        in_specs=(
            P(("grp", "rep"), None),
            P(("grp", "rep"), None),
            P(("grp", "rep"), None),
            P(),
            P("grp", None),
        ),
        out_specs=(P("grp", None), P(("grp", "rep"), None)),
        check_vma=False,
    )
```

```python
import jax
import jax.numpy as jnp
from jax import lax
from jax.experimental import pallas as pl
from jax.experimental.pallas import tpu as pltpu
from jax.sharding import PartitionSpec as P

LANES = 128
VMEM_LIMIT = 24 * 2**20
F32 = jnp.float32
BF16 = jnp.bfloat16


def iota(shape, dim):
    return lax.broadcasted_iota(jnp.int32, shape, dim)


def ones_where(mask):
    return jnp.where(mask, F32(1), F32(0)).astype(BF16)


def dot(a, b, contract=(1, 0)):
    return lax.dot_general(
        a, b, (((contract[0],), (contract[1],)), ((), ())), preferred_element_type=F32
    )


def pieces(value, count):
    result = []
    for _ in range(count):
        part = value.astype(BF16)
        result.append(part)
        value = value - part.astype(F32)
    return result


def each(count, fn, axis):
    return jnp.concatenate([fn(k) for k in range(count)], axis=axis)


def route_kernel(
    ids_hbm, weight_hbm, table_hbm, vectors_hbm, send_ref, seat_ref, ids_ref, weight_ref, table_ref,
    vectors_ref, sems, *, cap, lists_here,
):
    copies = [
        pltpu.make_async_copy(source, target, sems.at[i])
        for i, (source, target) in enumerate(
            [(ids_hbm, ids_ref), (table_hbm, table_ref), (weight_hbm, weight_ref), (vectors_hbm, vectors_ref)]
        )
    ]
    for copy in copies:
        copy.start()
    slots, rows = ids_ref.shape
    feature_dim = vectors_ref.shape[1]
    half = cap // 2
    sent = send_ref.shape[0]
    owners = sent // half
    copies[0].wait()
    ids = ids_ref[...]
    live = ids >= 0
    safe = jnp.maximum(ids, 0)
    high, low = safe >> 7, safe & 127
    row_of_table = iota((table_ref.shape[0], rows), 0)
    picks = each(slots, lambda k: ones_where(row_of_table == high[k : k + 1]), 1)
    copies[1].wait()
    table = table_ref[...]
    digits = jnp.concatenate(
        [(table >> 8).astype(F32).astype(BF16), (table & 255).astype(F32).astype(BF16)], axis=1
    )
    found = dot(digits, picks, (0, 0))
    found = found[:LANES] * 256 + found[LANES:]
    lane_of_table = iota((LANES, rows), 0)
    place = each(
        slots,
        lambda k: jnp.sum(
            jnp.where(lane_of_table == low[k : k + 1], found[:, k * rows : (k + 1) * rows], 0.0),
            axis=0,
            keepdims=True,
        ),
        0,
    ).astype(jnp.int32)
    copies[2].wait()
    owner = jnp.where(live, place // lists_here, owners)
    code = (place % lists_here) * 8 + weight_ref[...]

    owner_iota = iota((owners, rows), 0)
    at_owner = [owner_iota == owner[k : k + 1] for k in range(slots)]
    before = ones_where(iota((rows, 2 * rows), 0) < iota((rows, 2 * rows), 1))
    counted = dot(each(slots, lambda k: ones_where(at_owner[k]), 0), before)
    carried = jnp.zeros((owners, rows), F32)
    ranks = []
    for k in range(slots):
        here = counted[k * owners : (k + 1) * owners]
        rank = jnp.where(at_owner[k], here[:, :rows] + carried, 0.0)
        ranks.append(jnp.sum(rank, axis=0, keepdims=True))
        carried = carried + here[:, rows:]
    rank = jnp.concatenate(ranks, axis=0).astype(jnp.int32)
    seat = jnp.where(live, (rank % 2) * sent + owner * half + rank // 2, -1)
    seat_ref[...] = seat

    seat_iota = iota((2 * sent, rows), 0)
    taken = jnp.zeros((2 * sent, rows), F32)
    codes = jnp.zeros((2 * sent, rows), jnp.int32)
    for k in range(slots):
        match = seat_iota == seat[k : k + 1]
        taken = jnp.where(match, 1.0, taken)
        codes = jnp.where(match, code[k : k + 1], codes)
    copies[3].wait()
    vectors = vectors_ref[...]
    taken = taken.astype(BF16)
    first = (codes >> 6).astype(F32).astype(BF16)
    second = (codes & 63).astype(F32).astype(BF16)
    for b in range(2):
        send_ref[:, b * feature_dim : (b + 1) * feature_dim] = dot(
            taken[b * sent : (b + 1) * sent], vectors
        ).astype(BF16)
    meta = jnp.concatenate([first[:sent], second[:sent], first[sent:], second[sent:]], axis=1)
    columns = send_ref.shape[1] - 2 * feature_dim
    spread = ones_where(iota((4 * rows, columns), 0) // rows == iota((4 * rows, columns), 1))
    send_ref[:, 2 * feature_dim :] = dot(meta, spread).astype(BF16)


def seat_vectors(got_ref, feature_dim):
    return each(2, lambda b: got_ref[:, b * feature_dim : (b + 1) * feature_dim], 0)


def sums_of(got_ref, centroids_high, centroids_low):
    lists_here, feature_dim = centroids_high.shape
    meta = got_ref[:, 2 * feature_dim :]
    vectors = seat_vectors(got_ref, feature_dim)
    seats = vectors.shape[0]
    columns = meta.astype(F32)
    code = each(
        2, lambda b: columns[:, 2 * b : 2 * b + 1] * 64 + columns[:, 2 * b + 1 : 2 * b + 2], 0
    ).astype(jnp.int32)
    chosen = ones_where(iota((seats, lists_here), 1) == (code >> 3))
    to_rows = ones_where(iota((8, LANES), 0) == iota((8, LANES), 1))
    rows = dot(to_rows, meta, (1, 1))
    list_row = (
        each(2, lambda b: rows[2 * b : 2 * b + 1] * 64 + rows[2 * b + 1 : 2 * b + 2], 1).astype(jnp.int32)
        >> 3
    )
    named = iota((lists_here, seats), 0) == list_row

    centre = dot(chosen, centroids_high) + dot(chosen, centroids_low)
    sq_norms = jnp.sum((vectors.astype(F32) - centre) ** 2, axis=1, keepdims=True)
    shares = (code & 7).astype(F32) / (1.0 + sq_norms / feature_dim)
    high, low = pieces(shares, 2)
    lane = iota((seats, LANES), 1)
    block = jnp.where(lane == 0, high.astype(F32), jnp.where(lane == 1, low.astype(F32), 0.0))
    share_rows = dot(to_rows, block.astype(BF16), (1, 1))
    parts = [jnp.where(named, share_rows[i : i + 1], 0.0) for i in range(2)]
    sums = sum(dot(part.astype(BF16), vectors) for part in parts)
    totals = jnp.sum(parts[0] + parts[1], axis=1, keepdims=True)
    return chosen, sums, totals


def own_sums_kernel(got_ref, centroids_ref, sums_ref, totals_ref, chosen_ref, high_ref, low_ref):
    high, low = pieces(centroids_ref[...], 2)
    high_ref[...] = high
    low_ref[...] = low
    chosen, sums, totals = sums_of(got_ref, high, low)
    chosen_ref[...] = chosen
    sums_ref[...] = sums
    totals_ref[...] = jnp.broadcast_to(totals, totals_ref.shape)


def refine_kernel(
    sums_ref, totals_ref, chosen_ref, peer_ref, got_ref, high_ref, low_ref, centroids_ref, refined_hbm,
    dist_ref, refined_ref, sem, *, cap,
):
    lists_here, feature_dim = centroids_ref.shape
    _, peer_sums, peer_totals = sums_of(peer_ref, high_ref[...], low_ref[...])
    scale = 1.0 / (1.0 + (totals_ref[:, 0:1] + peer_totals))
    refined = (centroids_ref[...] + (sums_ref[...] + peer_sums)) * scale
    refined_ref[...] = refined
    copy = pltpu.make_async_copy(refined_ref, refined_hbm, sem)
    copy.start()
    chosen = chosen_ref[...]
    centre = sum(dot(chosen, part) for part in pieces(refined, 2))
    vectors = seat_vectors(got_ref, feature_dim).astype(F32)
    dist = jnp.sum((vectors - centre) ** 2, axis=1, keepdims=True) / feature_dim
    half = cap // 2
    sent = got_ref.shape[0]
    owners = sent // half
    seat, lane = iota((2 * sent, LANES), 0), iota((2 * sent, LANES), 1)
    spread = jnp.where((seat % half) * 2 + seat // sent == lane, dist, 0.0)
    gather = ones_where((iota((owners, 2 * sent), 1) % sent) // half == iota((owners, 2 * sent), 0))
    dist_ref[...] = sum(dot(gather, part) for part in pieces(spread, 3))
    copy.wait()


def pick_kernel(dist_ref, seat_ref, out_ref, *, cap):
    slots, rows = seat_ref.shape
    owners = dist_ref.shape[0]
    half = cap // 2
    sent = owners * half
    seat = seat_ref[...]
    owner = jnp.where(seat >= 0, (seat % sent) // half, owners)
    rank = (seat % half) * 2 + seat // sent
    by_rank = dist_ref[...].T[:8]
    owner_iota = iota((owners, rows), 0)
    at_owner = each(slots, lambda k: ones_where(owner_iota == owner[k : k + 1]), 1)
    found = sum(dot(part, at_owner) for part in pieces(by_rank, 3))
    rank_iota = iota((8, rows), 0)
    picked = each(
        slots,
        lambda k: jnp.sum(
            jnp.where(rank_iota == rank[k : k + 1], found[:, k * rows : (k + 1) * rows], 0.0),
            axis=0,
            keepdims=True,
        ),
        0,
    )
    out_ref[...] = jnp.where(seat >= 0, picked, 0.0)


def on_chip(kernel, outs, *args, name, in_hbm=(), out_hbm=(), scratch=()):
    def spec(i, away):
        return pl.BlockSpec(memory_space=pltpu.HBM if i in away else pltpu.VMEM)

    args = [
        pltpu.with_memory_space_constraint(a, pltpu.HBM) if i in in_hbm else a
        for i, a in enumerate(args)
    ]

    return pl.pallas_call(
        kernel,
        out_shape=outs,
        in_specs=[spec(i, in_hbm) for i in range(len(args))],
        out_specs=[spec(i, out_hbm) for i in range(len(outs))],
        scratch_shapes=list(scratch),
        compiler_params=pltpu.CompilerParams(vmem_limit_bytes=VMEM_LIMIT),
        name=name,
    )(*args)


def shards(vectors, list_ids, spill_weight, list_pos, old_centroids):
    owners = lax.axis_size("grp")
    row_count, slot_count = list_ids.shape
    lists_here, feature_dim = old_centroids.shape
    cap = row_count * slot_count // (2 * owners)
    half = cap // 2
    sent = owners * half
    width = 2 * feature_dim + LANES
    struct = jax.ShapeDtypeStruct

    inputs = (list_ids.T, spill_weight.T, list_pos.reshape(-1, LANES), vectors)
    send, seat = on_chip(
        lambda *refs: route_kernel(*refs, cap=cap, lists_here=lists_here),
        (struct((sent, width), BF16), struct((slot_count, row_count), jnp.int32)),
        *inputs,
        name="route",
        in_hbm=range(4),
        scratch=[
            *(pltpu.VMEM(a.shape, a.dtype) for a in inputs),
            pltpu.SemaphoreType.DMA((4,)),
        ],
    )
    got = lax.all_to_all(send.reshape(owners, half, width), "grp", 0, 0, tiled=True)
    got = got.reshape(sent, width)
    peer = lax.ppermute(got, "rep", [(0, 1), (1, 0)])
    sums, totals, chosen, high, low = on_chip(
        own_sums_kernel,
        (
            struct((lists_here, feature_dim), F32),
            struct((lists_here, LANES), F32),
            struct((2 * sent, lists_here), BF16),
            struct((lists_here, feature_dim), BF16),
            struct((lists_here, feature_dim), BF16),
        ),
        got,
        old_centroids,
        name="own_sums",
    )
    refined, owner_dist = on_chip(
        lambda *refs: refine_kernel(*refs, cap=cap),
        (struct((lists_here, feature_dim), F32), struct((owners, LANES), F32)),
        sums,
        totals,
        chosen,
        peer,
        got,
        high,
        low,
        old_centroids,
        name="refine",
        out_hbm=(0,),
        scratch=[pltpu.VMEM((lists_here, feature_dim), F32), pltpu.SemaphoreType.DMA],
    )
    seat_dist = lax.all_to_all(owner_dist.reshape(owners, 1, LANES), "grp", 0, 0, tiled=True)
    (new_dist,) = on_chip(
        lambda *refs: pick_kernel(*refs, cap=cap),
        (struct((slot_count, row_count), F32),),
        seat_dist.reshape(owners, LANES),
        seat,
        name="pick",
    )
    return refined, new_dist.T


def solution(mesh):
    return jax.shard_map(
        shards,
        mesh=mesh,
        in_specs=(
            P(("grp", "rep"), None),
            P(("grp", "rep"), None),
            P(("grp", "rep"), None),
            P(),
            P("grp", None),
        ),
        out_specs=(P("grp", None), P(("grp", "rep"), None)),
        check_vma=False,
    )
```

```python
import jax
import jax.numpy as jnp
from jax import lax
from jax.experimental import pallas as pl
from jax.experimental.pallas import tpu as pltpu
from jax.sharding import PartitionSpec as P

LANES = 128
CHUNK = 256
VMEM_LIMIT = 24 * 2**20
F32 = jnp.float32
BF16 = jnp.bfloat16


def iota(shape, dim):
    return lax.broadcasted_iota(jnp.int32, shape, dim)


def ones_where(mask):
    return jnp.where(mask, F32(1), F32(0)).astype(BF16)


def dot(a, b, contract=(1, 0)):
    return lax.dot_general(
        a, b, (((contract[0],), (contract[1],)), ((), ())), preferred_element_type=F32
    )


def pieces(value, count):
    result = []
    for _ in range(count):
        part = value.astype(BF16)
        result.append(part)
        value = value - part.astype(F32)
    return result


def each(count, fn, axis):
    return jnp.concatenate([fn(k) for k in range(count)], axis=axis)


def route_kernel(
    ids_hbm, weight_hbm, table_hbm, vectors_hbm, send_ref, seat_ref, ids_ref, weight_ref, table_ref,
    vectors_ref, sems, *, cap, lists_here,
):
    copies = [
        pltpu.make_async_copy(source, target, sems.at[i])
        for i, (source, target) in enumerate(
            [(ids_hbm, ids_ref), (table_hbm, table_ref), (weight_hbm, weight_ref), (vectors_hbm, vectors_ref)]
        )
    ]
    for copy in copies:
        copy.start()
    slots, rows = ids_ref.shape
    feature_dim = vectors_ref.shape[1]
    half = cap // 2
    sent = send_ref.shape[0]
    owners = sent // half
    copies[0].wait()
    ids = ids_ref[...]
    live = ids >= 0
    safe = jnp.maximum(ids, 0)
    high, low = safe >> 7, safe & 127
    row_of_table = iota((table_ref.shape[0], rows), 0)
    picks = each(slots, lambda k: ones_where(row_of_table == high[k : k + 1]), 1)
    copies[1].wait()
    table = table_ref[...]
    digits = jnp.concatenate(
        [(table >> 8).astype(F32).astype(BF16), (table & 255).astype(F32).astype(BF16)], axis=1
    )
    found = dot(digits, picks, (0, 0))
    found = found[:LANES] * 256 + found[LANES:]
    lane_of_table = iota((LANES, rows), 0)
    place = each(
        slots,
        lambda k: jnp.sum(
            jnp.where(lane_of_table == low[k : k + 1], found[:, k * rows : (k + 1) * rows], 0.0),
            axis=0,
            keepdims=True,
        ),
        0,
    ).astype(jnp.int32)
    copies[2].wait()
    owner = jnp.where(live, place // lists_here, owners)
    code = (place % lists_here) * 8 + weight_ref[...]

    owner_iota = iota((owners, rows), 0)
    at_owner = [owner_iota == owner[k : k + 1] for k in range(slots)]
    before = ones_where(iota((rows, 2 * rows), 0) < iota((rows, 2 * rows), 1))
    counted = dot(each(slots, lambda k: ones_where(at_owner[k]), 0), before)
    carried = jnp.zeros((owners, rows), F32)
    ranks = []
    for k in range(slots):
        here = counted[k * owners : (k + 1) * owners]
        rank = jnp.where(at_owner[k], here[:, :rows] + carried, 0.0)
        ranks.append(jnp.sum(rank, axis=0, keepdims=True))
        carried = carried + here[:, rows:]
    rank = jnp.concatenate(ranks, axis=0).astype(jnp.int32)
    seat = jnp.where(live, (rank % 2) * sent + owner * half + rank // 2, -1)
    seat_ref[...] = seat

    seat_iota = iota((2 * sent, rows), 0)
    taken = jnp.zeros((2 * sent, rows), F32)
    codes = jnp.zeros((2 * sent, rows), jnp.int32)
    for k in range(slots):
        match = seat_iota == seat[k : k + 1]
        taken = jnp.where(match, 1.0, taken)
        codes = jnp.where(match, code[k : k + 1], codes)
    copies[3].wait()
    vectors = vectors_ref[...]
    taken = taken.astype(BF16)
    first = (codes >> 6).astype(F32).astype(BF16)
    second = (codes & 63).astype(F32).astype(BF16)
    for b in range(2):
        send_ref[:, b * feature_dim : (b + 1) * feature_dim] = dot(
            taken[b * sent : (b + 1) * sent], vectors
        ).astype(BF16)
    meta = jnp.concatenate([first[:sent], second[:sent], first[sent:], second[sent:]], axis=1)
    columns = send_ref.shape[1] - 2 * feature_dim
    spread = ones_where(iota((4 * rows, columns), 0) // rows == iota((4 * rows, columns), 1))
    send_ref[:, 2 * feature_dim :] = dot(meta, spread).astype(BF16)


def seat_vectors(got_ref, feature_dim, chunk):
    return each(2, lambda b: got_ref[:, b * feature_dim + chunk.start : b * feature_dim + chunk.stop], 0)


def chunks_of(feature_dim):
    return [slice(at, at + CHUNK) for at in range(0, feature_dim, CHUNK)]


def folded(square):
    return sum(square[:, at : at + LANES] for at in range(0, square.shape[1], LANES))


def own_shares_kernel(got_ref, centroids_ref, chosen_ref, rows_ref):
    lists_here, feature_dim = centroids_ref.shape
    meta = got_ref[:, 2 * feature_dim :]
    columns = meta.astype(F32)
    code = each(
        2, lambda b: columns[:, 2 * b : 2 * b + 1] * 64 + columns[:, 2 * b + 1 : 2 * b + 2], 0
    ).astype(jnp.int32)
    seats = code.shape[0]
    chosen = ones_where(iota((seats, lists_here), 1) == (code >> 3))
    chosen_ref[...] = chosen
    total = jnp.zeros((seats, LANES), F32)
    for chunk in chunks_of(feature_dim):
        centre = sum(dot(chosen, part) for part in pieces(centroids_ref[:, chunk], 2))
        total = total + folded((seat_vectors(got_ref, feature_dim, chunk).astype(F32) - centre) ** 2)
    sq_norms = jnp.sum(total, axis=1, keepdims=True)
    shares = (code & 7).astype(F32) / (1.0 + sq_norms / feature_dim)
    high, low = pieces(shares, 2)
    lists = code >> 3
    lane = iota((seats, LANES), 1)
    block = jnp.where(lane == 0, high.astype(F32), jnp.where(lane == 1, low.astype(F32), 0.0))
    block = jnp.where(lane == 2, (lists >> 8).astype(F32), block)
    block = jnp.where(lane == 3, (lists & 255).astype(F32), block)
    to_rows = ones_where(iota((8, LANES), 0) == iota((8, LANES), 1))
    rows = dot(to_rows, block.astype(BF16), (1, 1))
    row = iota((8, seats), 0)
    rows_ref[...] = jnp.where(row == 2, rows[2:3] * 256 + rows[3:4], rows)


def placed(rows_ref, lists_here):
    rows = rows_ref[...]
    named = iota((lists_here, rows.shape[1]), 0) == rows[2:3].astype(jnp.int32)
    parts = [jnp.where(named, rows[i : i + 1], 0.0) for i in range(2)]
    totals = jnp.sum(parts[0] + parts[1], axis=1, keepdims=True)
    return [part.astype(BF16) for part in parts], totals


def own_sums_kernel(got_ref, rows_ref, sums_ref, totals_ref):
    lists_here, feature_dim = sums_ref.shape
    parts, totals = placed(rows_ref, lists_here)
    totals_ref[...] = jnp.broadcast_to(totals, totals_ref.shape)
    for chunk in chunks_of(feature_dim):
        vectors = seat_vectors(got_ref, feature_dim, chunk)
        sums_ref[:, chunk] = sum(dot(part, vectors) for part in parts)


def refine_kernel(
    sums_ref, totals_ref, chosen_ref, peer_ref, peer_rows_ref, got_ref, centroids_ref, refined_hbm,
    dist_ref, refined_ref, sem, *, cap,
):
    lists_here, feature_dim = centroids_ref.shape
    parts, peer_totals = placed(peer_rows_ref, lists_here)
    scale = 1.0 / (1.0 + (totals_ref[:, 0:1] + peer_totals))
    chunks = chunks_of(feature_dim)
    for chunk in chunks:
        vectors = seat_vectors(peer_ref, feature_dim, chunk)
        sums = sums_ref[:, chunk] + sum(dot(part, vectors) for part in parts)
        refined_ref[:, chunk] = (centroids_ref[:, chunk] + sums) * scale
    copy = pltpu.make_async_copy(refined_ref, refined_hbm, sem)
    copy.start()
    chosen = chosen_ref[...]
    half = cap // 2
    sent = got_ref.shape[0]
    owners = sent // half
    total = jnp.zeros((2 * sent, LANES), F32)
    for chunk in chunks:
        centre = sum(dot(chosen, part) for part in pieces(refined_ref[:, chunk], 2))
        total = total + folded((seat_vectors(got_ref, feature_dim, chunk).astype(F32) - centre) ** 2)
    dist = jnp.sum(total, axis=1, keepdims=True) / feature_dim
    seat, lane = iota((2 * sent, LANES), 0), iota((2 * sent, LANES), 1)
    spread = jnp.where((seat % half) * 2 + seat // sent == lane, dist, 0.0)
    gather = ones_where((iota((owners, 2 * sent), 1) % sent) // half == iota((owners, 2 * sent), 0))
    dist_ref[...] = sum(dot(gather, part) for part in pieces(spread, 3))
    copy.wait()


def pick_kernel(dist_ref, seat_ref, out_ref, *, cap):
    slots, rows = seat_ref.shape
    owners = dist_ref.shape[0]
    half = cap // 2
    sent = owners * half
    seat = seat_ref[...]
    owner = jnp.where(seat >= 0, (seat % sent) // half, owners)
    rank = (seat % half) * 2 + seat // sent
    by_rank = dist_ref[...].T[:8]
    owner_iota = iota((owners, rows), 0)
    at_owner = each(slots, lambda k: ones_where(owner_iota == owner[k : k + 1]), 1)
    found = sum(dot(part, at_owner) for part in pieces(by_rank, 3))
    rank_iota = iota((8, rows), 0)
    picked = each(
        slots,
        lambda k: jnp.sum(
            jnp.where(rank_iota == rank[k : k + 1], found[:, k * rows : (k + 1) * rows], 0.0),
            axis=0,
            keepdims=True,
        ),
        0,
    )
    out_ref[...] = jnp.where(seat >= 0, picked, 0.0)


def on_chip(kernel, outs, *args, name, in_hbm=(), out_hbm=(), scratch=()):
    def spec(i, away):
        return pl.BlockSpec(memory_space=pltpu.HBM if i in away else pltpu.VMEM)

    args = [
        pltpu.with_memory_space_constraint(a, pltpu.HBM) if i in in_hbm else a
        for i, a in enumerate(args)
    ]

    return pl.pallas_call(
        kernel,
        out_shape=outs,
        in_specs=[spec(i, in_hbm) for i in range(len(args))],
        out_specs=[spec(i, out_hbm) for i in range(len(outs))],
        scratch_shapes=list(scratch),
        compiler_params=pltpu.CompilerParams(vmem_limit_bytes=VMEM_LIMIT),
        name=name,
    )(*args)


def shards(vectors, list_ids, spill_weight, list_pos, old_centroids):
    owners = lax.axis_size("grp")
    row_count, slot_count = list_ids.shape
    lists_here, feature_dim = old_centroids.shape
    cap = row_count * slot_count // (2 * owners)
    half = cap // 2
    sent = owners * half
    width = 2 * feature_dim + LANES
    struct = jax.ShapeDtypeStruct

    inputs = (list_ids.T, spill_weight.T, list_pos.reshape(-1, LANES), vectors)
    send, seat = on_chip(
        lambda *refs: route_kernel(*refs, cap=cap, lists_here=lists_here),
        (struct((sent, width), BF16), struct((slot_count, row_count), jnp.int32)),
        *inputs,
        name="route",
        in_hbm=range(4),
        scratch=[
            *(pltpu.VMEM(a.shape, a.dtype) for a in inputs),
            pltpu.SemaphoreType.DMA((4,)),
        ],
    )
    got = lax.all_to_all(send.reshape(owners, half, width), "grp", 0, 0, tiled=True)
    got = got.reshape(sent, width)
    swap = [(0, 1), (1, 0)]
    peer = lax.ppermute(got, "rep", swap)
    chosen, rows = on_chip(
        own_shares_kernel,
        (struct((2 * sent, lists_here), BF16), struct((8, 2 * sent), F32)),
        got,
        old_centroids,
        name="own_shares",
    )
    peer_rows = lax.ppermute(rows, "rep", swap)
    sums, totals = on_chip(
        own_sums_kernel,
        (struct((lists_here, feature_dim), F32), struct((lists_here, LANES), F32)),
        got,
        rows,
        name="own_sums",
    )
    refined, owner_dist = on_chip(
        lambda *refs: refine_kernel(*refs, cap=cap),
        (struct((lists_here, feature_dim), F32), struct((owners, LANES), F32)),
        sums,
        totals,
        chosen,
        peer,
        peer_rows,
        got,
        old_centroids,
        name="refine",
        out_hbm=(0,),
        scratch=[pltpu.VMEM((lists_here, feature_dim), F32), pltpu.SemaphoreType.DMA],
    )
    seat_dist = lax.all_to_all(owner_dist.reshape(owners, 1, LANES), "grp", 0, 0, tiled=True)
    (new_dist,) = on_chip(
        lambda *refs: pick_kernel(*refs, cap=cap),
        (struct((slot_count, row_count), F32),),
        seat_dist.reshape(owners, LANES),
        seat,
        name="pick",
    )
    return refined, new_dist.T


def solution(mesh):
    return jax.shard_map(
        shards,
        mesh=mesh,
        in_specs=(
            P(("grp", "rep"), None),
            P(("grp", "rep"), None),
            P(("grp", "rep"), None),
            P(),
            P("grp", None),
        ),
        out_specs=(P("grp", None), P(("grp", "rep"), None)),
        check_vma=False,
    )
```

```python
import jax
import jax.numpy as jnp
from jax import lax
from jax.experimental import pallas as pl
from jax.experimental.pallas import tpu as pltpu
from jax.sharding import PartitionSpec as P

LANES = 128
CHUNK = 256
VMEM_LIMIT = 24 * 2**20
F32 = jnp.float32
BF16 = jnp.bfloat16


def iota(shape, dim):
    return lax.broadcasted_iota(jnp.int32, shape, dim)


def ones_where(mask):
    return jnp.where(mask, F32(1), F32(0)).astype(BF16)


def dot(a, b, contract=(1, 0)):
    return lax.dot_general(
        a, b, (((contract[0],), (contract[1],)), ((), ())), preferred_element_type=F32
    )


def pieces(value, count):
    result = []
    for _ in range(count):
        part = value.astype(BF16)
        result.append(part)
        value = value - part.astype(F32)
    return result


def dot_of_pieces(a, parts):
    return dot(jnp.concatenate([a] * len(parts), axis=1), jnp.concatenate(parts, axis=0))


def each(count, fn, axis):
    return jnp.concatenate([fn(k) for k in range(count)], axis=axis)


def route_kernel(
    ids_hbm, weight_hbm, table_hbm, vectors_hbm, send_ref, seat_ref, ids_ref, weight_ref, table_ref,
    vectors_ref, sems, *, cap, lists_here,
):
    copies = [
        pltpu.make_async_copy(source, target, sems.at[i])
        for i, (source, target) in enumerate(
            [(ids_hbm, ids_ref), (table_hbm, table_ref), (weight_hbm, weight_ref), (vectors_hbm, vectors_ref)]
        )
    ]
    for copy in copies:
        copy.start()
    slots, rows = ids_ref.shape
    feature_dim = vectors_ref.shape[1]
    half = cap // 2
    sent = send_ref.shape[0]
    owners = sent // half
    copies[0].wait()
    ids = ids_ref[...]
    live = ids >= 0
    safe = jnp.maximum(ids, 0)
    high, low = safe >> 7, safe & 127
    row_of_table = iota((table_ref.shape[0], rows), 0)
    picks = each(slots, lambda k: ones_where(row_of_table == high[k : k + 1]), 1)
    copies[1].wait()
    table = table_ref[...]
    digits = jnp.concatenate(
        [(table >> 8).astype(F32).astype(BF16), (table & 255).astype(F32).astype(BF16)], axis=1
    )
    found = dot(digits, picks, (0, 0))
    found = found[:LANES] * 256 + found[LANES:]
    lane_of_table = iota((LANES, rows), 0)
    place = each(
        slots,
        lambda k: jnp.sum(
            jnp.where(lane_of_table == low[k : k + 1], found[:, k * rows : (k + 1) * rows], 0.0),
            axis=0,
            keepdims=True,
        ),
        0,
    ).astype(jnp.int32)
    copies[2].wait()
    owner = jnp.where(live, place // lists_here, owners)
    code = (place % lists_here) * 8 + weight_ref[...]

    owner_iota = iota((owners, rows), 0)
    at_owner = [owner_iota == owner[k : k + 1] for k in range(slots)]
    before = ones_where(iota((rows, 2 * rows), 0) < iota((rows, 2 * rows), 1))
    counted = dot(each(slots, lambda k: ones_where(at_owner[k]), 0), before)
    carried = jnp.zeros((owners, rows), F32)
    ranks = []
    for k in range(slots):
        here = counted[k * owners : (k + 1) * owners]
        rank = jnp.where(at_owner[k], here[:, :rows] + carried, 0.0)
        ranks.append(jnp.sum(rank, axis=0, keepdims=True))
        carried = carried + here[:, rows:]
    rank = jnp.concatenate(ranks, axis=0).astype(jnp.int32)
    seat = jnp.where(live, (rank % 2) * sent + owner * half + rank // 2, -1)
    seat_ref[...] = seat

    copies[3].wait()
    vectors = vectors_ref[...]
    columns = send_ref.shape[1] - 2 * feature_dim
    spread = ones_where(iota((4 * rows, columns), 0) // rows == iota((4 * rows, columns), 1))
    for at in range(0, sent, rows):
        here = slice(at, at + rows)
        digits = []
        for b in range(2):
            seat_iota = iota((rows, rows), 0) + (b * sent + at)
            codes = jnp.zeros((rows, rows), jnp.int32)
            for k in range(slots):
                codes = jnp.where(seat_iota == seat[k : k + 1], code[k : k + 1], codes)
            digits += [(codes >> 6).astype(F32).astype(BF16), (codes & 63).astype(F32).astype(BF16)]
            send_ref[here, b * feature_dim : (b + 1) * feature_dim] = dot(
                ones_where(codes > 0), vectors
            ).astype(BF16)
        send_ref[here, 2 * feature_dim :] = dot(jnp.concatenate(digits, axis=1), spread).astype(BF16)


def seat_vectors(got_ref, feature_dim, chunk):
    return each(2, lambda b: got_ref[:, b * feature_dim + chunk.start : b * feature_dim + chunk.stop], 0)


def chunks_of(feature_dim):
    return [slice(at, at + CHUNK) for at in range(0, feature_dim, CHUNK)]


def folded(square):
    return sum(square[:, at : at + LANES] for at in range(0, square.shape[1], LANES))


def own_shares_kernel(got_ref, centroids_ref, chosen_ref, rows_ref):
    lists_here, feature_dim = centroids_ref.shape
    meta = got_ref[:, 2 * feature_dim :]
    columns = meta.astype(F32)
    code = each(
        2, lambda b: columns[:, 2 * b : 2 * b + 1] * 64 + columns[:, 2 * b + 1 : 2 * b + 2], 0
    ).astype(jnp.int32)
    seats = code.shape[0]
    for at in range(0, seats, LANES):
        here = slice(at, at + LANES)
        chosen_ref[here] = ones_where(iota((LANES, lists_here), 1) == (code[here] >> 3))
    total = jnp.zeros((seats, LANES), F32)
    for chunk in chunks_of(feature_dim):
        centre = dot_of_pieces(chosen_ref[...], pieces(centroids_ref[:, chunk], 2))
        total = total + folded((seat_vectors(got_ref, feature_dim, chunk).astype(F32) - centre) ** 2)
    sq_norms = jnp.sum(total, axis=1, keepdims=True)
    shares = (code & 7).astype(F32) / (1.0 + sq_norms / feature_dim)
    high, low = pieces(shares, 2)
    lists = code >> 3
    lane = iota((seats, LANES), 1)
    block = jnp.where(lane == 0, high.astype(F32), jnp.where(lane == 1, low.astype(F32), 0.0))
    block = jnp.where(lane == 2, (lists >> 8).astype(F32), block)
    block = jnp.where(lane == 3, (lists & 255).astype(F32), block)
    to_rows = ones_where(iota((8, LANES), 0) == iota((8, LANES), 1))
    rows = dot(to_rows, block.astype(BF16), (1, 1))
    row = iota((8, seats), 0)
    rows_ref[...] = jnp.where(row == 2, rows[2:3] * 256 + rows[3:4], rows)


def placed(rows_ref, lists_here):
    rows = rows_ref[...]
    named = iota((lists_here, rows.shape[1]), 0) == rows[2:3].astype(jnp.int32)
    parts = [jnp.where(named, rows[i : i + 1], 0.0) for i in range(2)]
    totals = jnp.sum(parts[0] + parts[1], axis=1, keepdims=True)
    return jnp.concatenate([part.astype(BF16) for part in parts], axis=1), totals


def own_sums_kernel(got_ref, rows_ref, sums_ref, totals_ref):
    lists_here, feature_dim = sums_ref.shape
    parts, totals = placed(rows_ref, lists_here)
    totals_ref[...] = jnp.broadcast_to(totals, totals_ref.shape)
    for chunk in chunks_of(feature_dim):
        vectors = seat_vectors(got_ref, feature_dim, chunk)
        sums_ref[:, chunk] = dot(parts, jnp.concatenate([vectors] * 2, axis=0))


def refine_kernel(
    sums_ref, totals_ref, chosen_ref, peer_ref, peer_rows_ref, got_ref, centroids_ref, refined_hbm,
    dist_ref, refined_ref, seat_dist_ref, sem, *, cap,
):
    lists_here, feature_dim = centroids_ref.shape
    parts, peer_totals = placed(peer_rows_ref, lists_here)
    scale = 1.0 / (1.0 + (totals_ref[:, 0:1] + peer_totals))
    chunks = chunks_of(feature_dim)
    for chunk in chunks:
        vectors = seat_vectors(peer_ref, feature_dim, chunk)
        sums = sums_ref[:, chunk] + dot(parts, jnp.concatenate([vectors] * 2, axis=0))
        refined_ref[:, chunk] = (centroids_ref[:, chunk] + sums) * scale
    copy = pltpu.make_async_copy(refined_ref, refined_hbm, sem)
    copy.start()
    half = cap // 2
    sent = got_ref.shape[0]
    owners = sent // half
    total = jnp.zeros((2 * sent, LANES), F32)
    for chunk in chunks:
        centre = dot_of_pieces(chosen_ref[...], pieces(refined_ref[:, chunk], 2))
        total = total + folded((seat_vectors(got_ref, feature_dim, chunk).astype(F32) - centre) ** 2)
    dist = jnp.sum(total, axis=1, keepdims=True) / feature_dim
    seat_dist_ref[...] = jnp.broadcast_to(dist, seat_dist_ref.shape)
    lane = iota((owners, LANES), 1)
    by_owner = jnp.zeros((owners, LANES), F32)
    for a in range(half):
        for b in range(2):
            mine = seat_dist_ref[pl.ds(b * sent + a, owners, stride=half), :]
            by_owner = jnp.where(lane == 2 * a + b, mine, by_owner)
    dist_ref[...] = by_owner
    copy.wait()


def pick_kernel(dist_ref, seat_ref, out_ref, *, cap):
    slots, rows = seat_ref.shape
    owners = dist_ref.shape[0]
    half = cap // 2
    sent = owners * half
    seat = seat_ref[...]
    owner = jnp.where(seat >= 0, (seat % sent) // half, owners)
    rank = (seat % half) * 2 + seat // sent
    by_rank = dist_ref[...].T[:8]
    owner_iota = iota((owners, rows), 0)
    at_owner = each(slots, lambda k: ones_where(owner_iota == owner[k : k + 1]), 1)
    found = sum(dot(part, at_owner) for part in pieces(by_rank, 3))
    rank_iota = iota((8, rows), 0)
    picked = each(
        slots,
        lambda k: jnp.sum(
            jnp.where(rank_iota == rank[k : k + 1], found[:, k * rows : (k + 1) * rows], 0.0),
            axis=0,
            keepdims=True,
        ),
        0,
    )
    out_ref[...] = jnp.where(seat >= 0, picked, 0.0)


def on_chip(kernel, outs, *args, name, in_hbm=(), out_hbm=(), scratch=()):
    def spec(i, away):
        return pl.BlockSpec(memory_space=pltpu.HBM if i in away else pltpu.VMEM)

    args = [
        pltpu.with_memory_space_constraint(a, pltpu.HBM) if i in in_hbm else a
        for i, a in enumerate(args)
    ]

    return pl.pallas_call(
        kernel,
        out_shape=outs,
        in_specs=[spec(i, in_hbm) for i in range(len(args))],
        out_specs=[spec(i, out_hbm) for i in range(len(outs))],
        scratch_shapes=list(scratch),
        compiler_params=pltpu.CompilerParams(vmem_limit_bytes=VMEM_LIMIT),
        name=name,
    )(*args)


def shards(vectors, list_ids, spill_weight, list_pos, old_centroids):
    owners = lax.axis_size("grp")
    row_count, slot_count = list_ids.shape
    lists_here, feature_dim = old_centroids.shape
    cap = row_count * slot_count // (2 * owners)
    half = cap // 2
    sent = owners * half
    width = 2 * feature_dim + LANES
    struct = jax.ShapeDtypeStruct

    inputs = (list_ids.T, spill_weight.T, list_pos.reshape(-1, LANES), vectors)
    send, seat = on_chip(
        lambda *refs: route_kernel(*refs, cap=cap, lists_here=lists_here),
        (struct((sent, width), BF16), struct((slot_count, row_count), jnp.int32)),
        *inputs,
        name="route",
        in_hbm=range(4),
        scratch=[
            *(pltpu.VMEM(a.shape, a.dtype) for a in inputs),
            pltpu.SemaphoreType.DMA((4,)),
        ],
    )
    got = lax.all_to_all(send.reshape(owners, half, width), "grp", 0, 0, tiled=True)
    got = got.reshape(sent, width)
    swap = [(0, 1), (1, 0)]
    peer = lax.ppermute(got, "rep", swap)
    chosen, rows = on_chip(
        own_shares_kernel,
        (struct((2 * sent, lists_here), BF16), struct((8, 2 * sent), F32)),
        got,
        old_centroids,
        name="own_shares",
    )
    peer_rows = lax.ppermute(rows, "rep", swap)
    sums, totals = on_chip(
        own_sums_kernel,
        (struct((lists_here, feature_dim), F32), struct((lists_here, LANES), F32)),
        got,
        rows,
        name="own_sums",
    )
    refined, owner_dist = on_chip(
        lambda *refs: refine_kernel(*refs, cap=cap),
        (struct((lists_here, feature_dim), F32), struct((owners, LANES), F32)),
        sums,
        totals,
        chosen,
        peer,
        peer_rows,
        got,
        old_centroids,
        name="refine",
        out_hbm=(0,),
        scratch=[
            pltpu.VMEM((lists_here, feature_dim), F32),
            pltpu.VMEM((2 * sent, LANES), F32),
            pltpu.SemaphoreType.DMA,
        ],
    )
    seat_dist = lax.all_to_all(owner_dist.reshape(owners, 1, LANES), "grp", 0, 0, tiled=True)
    (new_dist,) = on_chip(
        lambda *refs: pick_kernel(*refs, cap=cap),
        (struct((slot_count, row_count), F32),),
        seat_dist.reshape(owners, LANES),
        seat,
        name="pick",
    )
    return refined, new_dist.T


def solution(mesh):
    return jax.shard_map(
        shards,
        mesh=mesh,
        in_specs=(
            P(("grp", "rep"), None),
            P(("grp", "rep"), None),
            P(("grp", "rep"), None),
            P(),
            P("grp", None),
        ),
        out_specs=(P("grp", None), P(("grp", "rep"), None)),
        check_vma=False,
    )
```

```python
import jax
import jax.numpy as jnp
from jax import lax
from jax.experimental import pallas as pl
from jax.experimental.pallas import tpu as pltpu
from jax.sharding import PartitionSpec as P

LANES = 128
CHUNK = 256
VMEM_LIMIT = 24 * 2**20
F32 = jnp.float32
BF16 = jnp.bfloat16


def iota(shape, dim):
    return lax.broadcasted_iota(jnp.int32, shape, dim)


def ones_where(mask):
    return jnp.where(mask, F32(1), F32(0)).astype(BF16)


def dot(a, b, contract=(1, 0)):
    return lax.dot_general(
        a, b, (((contract[0],), (contract[1],)), ((), ())), preferred_element_type=F32
    )


def pieces(value, count):
    result = []
    for _ in range(count):
        part = value.astype(BF16)
        result.append(part)
        value = value - part.astype(F32)
    return result


def dot_of_pieces(a, parts):
    return dot(jnp.concatenate([a] * len(parts), axis=1), jnp.concatenate(parts, axis=0))


def each(count, fn, axis):
    return jnp.concatenate([fn(k) for k in range(count)], axis=axis)


def route_kernel(
    ids_hbm, weight_hbm, table_hbm, vectors_hbm, send_ref, seat_ref, ids_ref, weight_ref, table_ref,
    vectors_ref, sems, *, cap, lists_here,
):
    copies = [
        pltpu.make_async_copy(source, target, sems.at[i])
        for i, (source, target) in enumerate(
            [(ids_hbm, ids_ref), (table_hbm, table_ref), (weight_hbm, weight_ref), (vectors_hbm, vectors_ref)]
        )
    ]
    for copy in copies:
        copy.start()
    slots, rows = ids_ref.shape
    feature_dim = vectors_ref.shape[1]
    half = cap // 2
    sent = send_ref.shape[0]
    owners = sent // half
    copies[0].wait()
    ids = ids_ref[...]
    live = ids >= 0
    safe = jnp.maximum(ids, 0)
    high, low = safe >> 7, safe & 127
    row_of_table = iota((table_ref.shape[0], rows), 0)
    picks = each(slots, lambda k: ones_where(row_of_table == high[k : k + 1]), 1)
    copies[1].wait()
    table = table_ref[...]
    digits = jnp.concatenate(
        [(table >> 8).astype(F32).astype(BF16), (table & 255).astype(F32).astype(BF16)], axis=1
    )
    found = dot(digits, picks, (0, 0))
    found = found[:LANES] * 256 + found[LANES:]
    lane_of_table = iota((LANES, rows), 0)
    place = each(
        slots,
        lambda k: jnp.sum(
            jnp.where(lane_of_table == low[k : k + 1], found[:, k * rows : (k + 1) * rows], 0.0),
            axis=0,
            keepdims=True,
        ),
        0,
    ).astype(jnp.int32)
    copies[2].wait()
    owner = jnp.where(live, place // lists_here, owners)
    code = (place % lists_here) * 8 + weight_ref[...]

    owner_iota = iota((owners, rows), 0)
    at_owner = [owner_iota == owner[k : k + 1] for k in range(slots)]
    before = ones_where(iota((rows, 2 * rows), 0) < iota((rows, 2 * rows), 1))
    counted = dot(each(slots, lambda k: ones_where(at_owner[k]), 0), before)
    carried = jnp.zeros((owners, rows), F32)
    ranks = []
    for k in range(slots):
        here = counted[k * owners : (k + 1) * owners]
        rank = jnp.where(at_owner[k], here[:, :rows] + carried, 0.0)
        ranks.append(jnp.sum(rank, axis=0, keepdims=True))
        carried = carried + here[:, rows:]
    rank = jnp.concatenate(ranks, axis=0).astype(jnp.int32)
    seat = jnp.where(live, (rank % 2) * sent + owner * half + rank // 2, -1)
    seat_ref[...] = seat

    copies[3].wait()
    vectors = vectors_ref[...]
    columns = send_ref.shape[1] - 2 * feature_dim
    spread = ones_where(iota((4 * rows, columns), 0) // rows == iota((4 * rows, columns), 1))
    for at in range(0, sent, rows):
        here = slice(at, at + rows)
        digits = []
        for b in range(2):
            seat_iota = iota((rows, rows), 0) + (b * sent + at)
            codes = jnp.zeros((rows, rows), jnp.int32)
            for k in range(slots):
                codes = jnp.where(seat_iota == seat[k : k + 1], code[k : k + 1], codes)
            digits += [(codes >> 6).astype(F32).astype(BF16), (codes & 63).astype(F32).astype(BF16)]
            send_ref[here, b * feature_dim : (b + 1) * feature_dim] = dot(
                ones_where(codes > 0), vectors
            ).astype(BF16)
        send_ref[here, 2 * feature_dim :] = dot(jnp.concatenate(digits, axis=1), spread).astype(BF16)


def seat_vectors(got_ref, feature_dim, chunk):
    return each(2, lambda b: got_ref[:, b * feature_dim + chunk.start : b * feature_dim + chunk.stop], 0)


def chunks_of(feature_dim):
    return [slice(at, at + CHUNK) for at in range(0, feature_dim, CHUNK)]


def folded(square):
    return sum(square[:, at : at + LANES] for at in range(0, square.shape[1], LANES))


def own_shares_kernel(got_ref, centroids_ref, chosen_ref, rows_ref):
    lists_here, feature_dim = centroids_ref.shape
    meta = got_ref[:, 2 * feature_dim :]
    columns = meta.astype(F32)
    code = each(
        2, lambda b: columns[:, 2 * b : 2 * b + 1] * 64 + columns[:, 2 * b + 1 : 2 * b + 2], 0
    ).astype(jnp.int32)
    seats = code.shape[0]
    for at in range(0, seats, LANES):
        here = slice(at, at + LANES)
        chosen_ref[here] = ones_where(iota((LANES, lists_here), 1) == (code[here] >> 3))
    to_rows = ones_where(iota((8, LANES), 0) == iota((8, LANES), 1))
    digits = dot(to_rows, meta, (1, 1))
    code_row = each(
        2, lambda b: digits[2 * b : 2 * b + 1] * 64 + digits[2 * b + 1 : 2 * b + 2], 1
    ).astype(jnp.int32)
    total = jnp.zeros((seats, LANES), F32)
    for chunk in chunks_of(feature_dim):
        centre = dot_of_pieces(chosen_ref[...], pieces(centroids_ref[:, chunk], 2))
        total = total + folded((seat_vectors(got_ref, feature_dim, chunk).astype(F32) - centre) ** 2)
    sq_norms = dot(jnp.ones((8, 3 * LANES), BF16), jnp.concatenate(pieces(total, 3), axis=1), (1, 1))
    shares = (code_row % 8).astype(F32) / (1.0 + sq_norms[0:1] / feature_dim)
    high, low = pieces(shares, 2)
    row = iota((8, seats), 0)
    rows_ref[...] = jnp.where(
        row == 0,
        high.astype(F32),
        jnp.where(row == 1, low.astype(F32), (code_row >> 3).astype(F32)),
    )


def placed(rows_ref, lists_here):
    rows = rows_ref[...]
    named = iota((lists_here, rows.shape[1]), 0) == rows[2:3].astype(jnp.int32)
    parts = [jnp.where(named, rows[i : i + 1], 0.0) for i in range(2)]
    totals = jnp.sum(parts[0] + parts[1], axis=1, keepdims=True)
    return jnp.concatenate([part.astype(BF16) for part in parts], axis=1), totals


def own_sums_kernel(got_ref, rows_ref, sums_ref, totals_ref):
    lists_here, feature_dim = sums_ref.shape
    parts, totals = placed(rows_ref, lists_here)
    totals_ref[...] = jnp.broadcast_to(totals, totals_ref.shape)
    for chunk in chunks_of(feature_dim):
        vectors = seat_vectors(got_ref, feature_dim, chunk)
        sums_ref[:, chunk] = dot(parts, jnp.concatenate([vectors] * 2, axis=0))


def refine_kernel(
    sums_ref, totals_ref, chosen_ref, peer_ref, peer_rows_ref, got_ref, centroids_ref, refined_hbm,
    dist_ref, refined_ref, seat_dist_ref, sem, *, cap,
):
    lists_here, feature_dim = centroids_ref.shape
    parts, peer_totals = placed(peer_rows_ref, lists_here)
    scale = 1.0 / (1.0 + (totals_ref[:, 0:1] + peer_totals))
    chunks = chunks_of(feature_dim)
    for chunk in chunks:
        vectors = seat_vectors(peer_ref, feature_dim, chunk)
        sums = sums_ref[:, chunk] + dot(parts, jnp.concatenate([vectors] * 2, axis=0))
        refined_ref[:, chunk] = (centroids_ref[:, chunk] + sums) * scale
    copy = pltpu.make_async_copy(refined_ref, refined_hbm, sem)
    copy.start()
    half = cap // 2
    sent = got_ref.shape[0]
    owners = sent // half
    total = jnp.zeros((2 * sent, LANES), F32)
    for chunk in chunks:
        centre = dot_of_pieces(chosen_ref[...], pieces(refined_ref[:, chunk], 2))
        total = total + folded((seat_vectors(got_ref, feature_dim, chunk).astype(F32) - centre) ** 2)
    dist = jnp.sum(total, axis=1, keepdims=True) / feature_dim
    seat_dist_ref[...] = jnp.broadcast_to(dist, seat_dist_ref.shape)
    lane = iota((owners, LANES), 1)
    by_owner = jnp.zeros((owners, LANES), F32)
    for a in range(half):
        for b in range(2):
            mine = seat_dist_ref[pl.ds(b * sent + a, owners, stride=half), :]
            by_owner = jnp.where(lane == 2 * a + b, mine, by_owner)
    dist_ref[...] = by_owner
    copy.wait()


def pick_kernel(dist_ref, seat_ref, out_ref, *, cap):
    slots, rows = seat_ref.shape
    owners = dist_ref.shape[0]
    half = cap // 2
    sent = owners * half
    seat = seat_ref[...]
    owner = jnp.where(seat >= 0, (seat % sent) // half, owners)
    rank = (seat % half) * 2 + seat // sent
    by_rank = dist_ref[...].T[:8]
    owner_iota = iota((owners, rows), 0)
    at_owner = each(slots, lambda k: ones_where(owner_iota == owner[k : k + 1]), 1)
    found = sum(dot(part, at_owner) for part in pieces(by_rank, 3))
    rank_iota = iota((8, rows), 0)
    picked = each(
        slots,
        lambda k: jnp.sum(
            jnp.where(rank_iota == rank[k : k + 1], found[:, k * rows : (k + 1) * rows], 0.0),
            axis=0,
            keepdims=True,
        ),
        0,
    )
    out_ref[...] = jnp.where(seat >= 0, picked, 0.0)


def on_chip(kernel, outs, *args, name, in_hbm=(), out_hbm=(), scratch=()):
    def spec(i, away):
        return pl.BlockSpec(memory_space=pltpu.HBM if i in away else pltpu.VMEM)

    args = [
        pltpu.with_memory_space_constraint(a, pltpu.HBM) if i in in_hbm else a
        for i, a in enumerate(args)
    ]

    return pl.pallas_call(
        kernel,
        out_shape=outs,
        in_specs=[spec(i, in_hbm) for i in range(len(args))],
        out_specs=[spec(i, out_hbm) for i in range(len(outs))],
        scratch_shapes=list(scratch),
        compiler_params=pltpu.CompilerParams(vmem_limit_bytes=VMEM_LIMIT),
        name=name,
    )(*args)


def shards(vectors, list_ids, spill_weight, list_pos, old_centroids):
    owners = lax.axis_size("grp")
    row_count, slot_count = list_ids.shape
    lists_here, feature_dim = old_centroids.shape
    cap = row_count * slot_count // (2 * owners)
    half = cap // 2
    sent = owners * half
    width = 2 * feature_dim + LANES
    struct = jax.ShapeDtypeStruct

    inputs = (list_ids.T, spill_weight.T, list_pos.reshape(-1, LANES), vectors)
    send, seat = on_chip(
        lambda *refs: route_kernel(*refs, cap=cap, lists_here=lists_here),
        (struct((sent, width), BF16), struct((slot_count, row_count), jnp.int32)),
        *inputs,
        name="route",
        in_hbm=range(4),
        scratch=[
            *(pltpu.VMEM(a.shape, a.dtype) for a in inputs),
            pltpu.SemaphoreType.DMA((4,)),
        ],
    )
    got = lax.all_to_all(send.reshape(owners, half, width), "grp", 0, 0, tiled=True)
    got = got.reshape(sent, width)
    swap = [(0, 1), (1, 0)]
    peer = lax.ppermute(got, "rep", swap)
    chosen, rows = on_chip(
        own_shares_kernel,
        (struct((2 * sent, lists_here), BF16), struct((8, 2 * sent), F32)),
        got,
        old_centroids,
        name="own_shares",
    )
    peer_rows = lax.ppermute(rows, "rep", swap)
    sums, totals = on_chip(
        own_sums_kernel,
        (struct((lists_here, feature_dim), F32), struct((lists_here, LANES), F32)),
        got,
        rows,
        name="own_sums",
    )
    refined, owner_dist = on_chip(
        lambda *refs: refine_kernel(*refs, cap=cap),
        (struct((lists_here, feature_dim), F32), struct((owners, LANES), F32)),
        sums,
        totals,
        chosen,
        peer,
        peer_rows,
        got,
        old_centroids,
        name="refine",
        out_hbm=(0,),
        scratch=[
            pltpu.VMEM((lists_here, feature_dim), F32),
            pltpu.VMEM((2 * sent, LANES), F32),
            pltpu.SemaphoreType.DMA,
        ],
    )
    seat_dist = lax.all_to_all(owner_dist.reshape(owners, 1, LANES), "grp", 0, 0, tiled=True)
    (new_dist,) = on_chip(
        lambda *refs: pick_kernel(*refs, cap=cap),
        (struct((slot_count, row_count), F32),),
        seat_dist.reshape(owners, LANES),
        seat,
        name="pick",
    )
    return refined, new_dist.T


def solution(mesh):
    return jax.shard_map(
        shards,
        mesh=mesh,
        in_specs=(
            P(("grp", "rep"), None),
            P(("grp", "rep"), None),
            P(("grp", "rep"), None),
            P(),
            P("grp", None),
        ),
        out_specs=(P("grp", None), P(("grp", "rep"), None)),
        check_vma=False,
    )
```

```python
import jax
import jax.numpy as jnp
from jax import lax
from jax.experimental import pallas as pl
from jax.experimental.pallas import tpu as pltpu
from jax.sharding import PartitionSpec as P

LANES = 128
CHUNK = 256
BLOCKS = 2
VMEM_LIMIT = 24 * 2**20
F32 = jnp.float32
BF16 = jnp.bfloat16


def iota(shape, dim):
    return lax.broadcasted_iota(jnp.int32, shape, dim)


def ones_where(mask):
    return jnp.where(mask, F32(1), F32(0)).astype(BF16)


def dot(a, b, contract=(1, 0)):
    return lax.dot_general(
        a, b, (((contract[0],), (contract[1],)), ((), ())), preferred_element_type=F32
    )


def pieces(value, count):
    result = []
    for _ in range(count):
        part = value.astype(BF16)
        result.append(part)
        value = value - part.astype(F32)
    return result


def dot_of_pieces(a, parts):
    return dot(jnp.concatenate([a] * len(parts), axis=1), jnp.concatenate(parts, axis=0))


def each(count, fn, axis):
    return jnp.concatenate([fn(k) for k in range(count)], axis=axis)


def route_kernel(
    ids_hbm, weight_hbm, table_hbm, vectors_hbm, send_ref, seat_ref, ids_ref, weight_ref, table_ref,
    vectors_ref, sems, *, cap, lists_here,
):
    copies = [
        pltpu.make_async_copy(source, target, sems.at[i])
        for i, (source, target) in enumerate(
            [(ids_hbm, ids_ref), (table_hbm, table_ref), (weight_hbm, weight_ref), (vectors_hbm, vectors_ref)]
        )
    ]
    for copy in copies:
        copy.start()
    slots, rows = ids_ref.shape
    feature_dim = vectors_ref.shape[1]
    half = cap // 2
    sent = send_ref.shape[0]
    owners = sent // half
    copies[0].wait()
    ids = ids_ref[...]
    live = ids >= 0
    safe = jnp.maximum(ids, 0)
    high, low = safe >> 7, safe & 127
    row_of_table = iota((table_ref.shape[0], rows), 0)
    picks = each(slots, lambda k: ones_where(row_of_table == high[k : k + 1]), 1)
    copies[1].wait()
    table = table_ref[...]
    digits = jnp.concatenate(
        [(table >> 8).astype(F32).astype(BF16), (table & 255).astype(F32).astype(BF16)], axis=1
    )
    found = dot(digits, picks, (0, 0))
    found = found[:LANES] * 256 + found[LANES:]
    lane_of_table = iota((LANES, rows), 0)
    place = each(
        slots,
        lambda k: jnp.sum(
            jnp.where(lane_of_table == low[k : k + 1], found[:, k * rows : (k + 1) * rows], 0.0),
            axis=0,
            keepdims=True,
        ),
        0,
    ).astype(jnp.int32)
    copies[2].wait()
    owner = jnp.where(live, place // lists_here, owners)
    code = (place % lists_here) * 8 + weight_ref[...]

    owner_iota = iota((owners, rows), 0)
    at_owner = [owner_iota == owner[k : k + 1] for k in range(slots)]
    before = ones_where(iota((rows, 2 * rows), 0) < iota((rows, 2 * rows), 1))
    counted = dot(each(slots, lambda k: ones_where(at_owner[k]), 0), before)
    carried = jnp.zeros((owners, rows), F32)
    ranks = []
    for k in range(slots):
        here = counted[k * owners : (k + 1) * owners]
        rank = jnp.where(at_owner[k], here[:, :rows] + carried, 0.0)
        ranks.append(jnp.sum(rank, axis=0, keepdims=True))
        carried = carried + here[:, rows:]
    rank = jnp.concatenate(ranks, axis=0).astype(jnp.int32)
    seat = jnp.where(live, (rank % 2) * sent + owner * half + rank // 2, -1)
    seat_ref[...] = seat

    copies[3].wait()
    vectors = vectors_ref[...]
    columns = send_ref.shape[1] - 2 * feature_dim
    spread = ones_where(iota((4 * rows, columns), 0) // rows == iota((4 * rows, columns), 1))
    for at in range(0, sent, rows):
        here = slice(at, at + rows)
        digits = []
        for b in range(2):
            seat_iota = iota((rows, rows), 0) + (b * sent + at)
            codes = jnp.zeros((rows, rows), jnp.int32)
            for k in range(slots):
                codes = jnp.where(seat_iota == seat[k : k + 1], code[k : k + 1], codes)
            digits += [(codes >> 6).astype(F32).astype(BF16), (codes & 63).astype(F32).astype(BF16)]
            send_ref[here, b * feature_dim : (b + 1) * feature_dim] = dot(
                ones_where(codes > 0), vectors
            ).astype(BF16)
        send_ref[here, 2 * feature_dim :] = dot(jnp.concatenate(digits, axis=1), spread).astype(BF16)


def seat_vectors(got_ref, feature_dim, chunk):
    return each(2, lambda b: got_ref[:, b * feature_dim + chunk.start : b * feature_dim + chunk.stop], 0)


def chunks_of(feature_dim):
    return [slice(at, at + CHUNK) for at in range(0, feature_dim, CHUNK)]


def folded(square):
    return sum(square[:, at : at + LANES] for at in range(0, square.shape[1], LANES))


def own_shares_kernel(got_ref, centroids_ref, chosen_ref, rows_ref):
    lists_here, feature_dim = centroids_ref.shape
    meta = got_ref[:, 2 * feature_dim :]
    columns = meta.astype(F32)
    code = each(
        2, lambda b: columns[:, 2 * b : 2 * b + 1] * 64 + columns[:, 2 * b + 1 : 2 * b + 2], 0
    ).astype(jnp.int32)
    seats = code.shape[0]
    for at in range(0, seats, LANES):
        here = slice(at, at + LANES)
        chosen_ref[here] = ones_where(iota((LANES, lists_here), 1) == (code[here] >> 3))
    to_rows = ones_where(iota((8, LANES), 0) == iota((8, LANES), 1))
    digits = dot(to_rows, meta, (1, 1))
    code_row = each(
        2, lambda b: digits[2 * b : 2 * b + 1] * 64 + digits[2 * b + 1 : 2 * b + 2], 1
    ).astype(jnp.int32)
    total = jnp.zeros((seats, LANES), F32)
    for chunk in chunks_of(feature_dim):
        centre = dot_of_pieces(chosen_ref[...], pieces(centroids_ref[:, chunk], 2))
        total = total + folded((seat_vectors(got_ref, feature_dim, chunk).astype(F32) - centre) ** 2)
    sq_norms = dot(jnp.ones((8, 3 * LANES), BF16), jnp.concatenate(pieces(total, 3), axis=1), (1, 1))
    shares = (code_row % 8).astype(F32) / (1.0 + sq_norms[0:1] / feature_dim)
    high, low = pieces(shares, 2)
    row = iota((8, seats), 0)
    rows_ref[...] = jnp.where(
        row == 0,
        high.astype(F32),
        jnp.where(row == 1, low.astype(F32), (code_row >> 3).astype(F32)),
    )


def placed(rows_ref, lists_here):
    rows = rows_ref[...]
    named = iota((lists_here, rows.shape[1]), 0) == rows[2:3].astype(jnp.int32)
    parts = [jnp.where(named, rows[i : i + 1], 0.0) for i in range(2)]
    totals = jnp.sum(parts[0] + parts[1], axis=1, keepdims=True)
    return jnp.concatenate([part.astype(BF16) for part in parts], axis=1), totals


def own_sums_kernel(got_ref, rows_ref, sums_ref, totals_ref):
    lists_here, feature_dim = sums_ref.shape
    parts, totals = placed(rows_ref, lists_here)
    totals_ref[...] = jnp.broadcast_to(totals, totals_ref.shape)
    for chunk in chunks_of(feature_dim):
        vectors = seat_vectors(got_ref, feature_dim, chunk)
        sums_ref[:, chunk] = dot(parts, jnp.concatenate([vectors] * 2, axis=0))


def refine_kernel(
    sums_ref, totals_ref, chosen_ref, peer_ref, peer_rows_ref, got_ref, centroids_ref, refined_hbm,
    dist_ref, refined_ref, seat_dist_ref, sems, *, cap,
):
    lists_here, feature_dim = centroids_ref.shape
    parts, peer_totals = placed(peer_rows_ref, lists_here)
    scale = 1.0 / (1.0 + (totals_ref[:, 0:1] + peer_totals))
    chunks = chunks_of(feature_dim)
    step = lists_here // BLOCKS
    copies = []
    for i in range(BLOCKS):
        here = slice(i * step, (i + 1) * step)
        for chunk in chunks:
            vectors = seat_vectors(peer_ref, feature_dim, chunk)
            sums = sums_ref[here, chunk] + dot(parts[here], jnp.concatenate([vectors] * 2, axis=0))
            refined_ref[here, chunk] = (centroids_ref[here, chunk] + sums) * scale[here]
        copies.append(
            pltpu.make_async_copy(refined_ref.at[here], refined_hbm.at[here], sems.at[i])
        )
        copies[-1].start()
    half = cap // 2
    sent = got_ref.shape[0]
    owners = sent // half
    total = jnp.zeros((2 * sent, LANES), F32)
    for chunk in chunks:
        centre = dot_of_pieces(chosen_ref[...], pieces(refined_ref[:, chunk], 2))
        total = total + folded((seat_vectors(got_ref, feature_dim, chunk).astype(F32) - centre) ** 2)
    dist = jnp.sum(total, axis=1, keepdims=True) / feature_dim
    seat_dist_ref[...] = jnp.broadcast_to(dist, seat_dist_ref.shape)
    lane = iota((owners, LANES), 1)
    by_owner = jnp.zeros((owners, LANES), F32)
    for a in range(half):
        for b in range(2):
            mine = seat_dist_ref[pl.ds(b * sent + a, owners, stride=half), :]
            by_owner = jnp.where(lane == 2 * a + b, mine, by_owner)
    dist_ref[...] = by_owner
    for copy in copies:
        copy.wait()


def pick_kernel(dist_ref, seat_ref, out_ref, *, cap):
    slots, rows = seat_ref.shape
    owners = dist_ref.shape[0]
    half = cap // 2
    sent = owners * half
    seat = seat_ref[...]
    owner = jnp.where(seat >= 0, (seat % sent) // half, owners)
    rank = (seat % half) * 2 + seat // sent
    by_rank = dist_ref[...].T[:8]
    owner_iota = iota((owners, rows), 0)
    at_owner = each(slots, lambda k: ones_where(owner_iota == owner[k : k + 1]), 1)
    found = sum(dot(part, at_owner) for part in pieces(by_rank, 3))
    rank_iota = iota((8, rows), 0)
    picked = each(
        slots,
        lambda k: jnp.sum(
            jnp.where(rank_iota == rank[k : k + 1], found[:, k * rows : (k + 1) * rows], 0.0),
            axis=0,
            keepdims=True,
        ),
        0,
    )
    out_ref[...] = jnp.where(seat >= 0, picked, 0.0)


def on_chip(kernel, outs, *args, name, in_hbm=(), out_hbm=(), scratch=()):
    def spec(i, away):
        return pl.BlockSpec(memory_space=pltpu.HBM if i in away else pltpu.VMEM)

    args = [
        pltpu.with_memory_space_constraint(a, pltpu.HBM) if i in in_hbm else a
        for i, a in enumerate(args)
    ]

    return pl.pallas_call(
        kernel,
        out_shape=outs,
        in_specs=[spec(i, in_hbm) for i in range(len(args))],
        out_specs=[spec(i, out_hbm) for i in range(len(outs))],
        scratch_shapes=list(scratch),
        compiler_params=pltpu.CompilerParams(vmem_limit_bytes=VMEM_LIMIT),
        name=name,
    )(*args)


def shards(vectors, list_ids, spill_weight, list_pos, old_centroids):
    owners = lax.axis_size("grp")
    row_count, slot_count = list_ids.shape
    lists_here, feature_dim = old_centroids.shape
    cap = row_count * slot_count // (2 * owners)
    half = cap // 2
    sent = owners * half
    width = 2 * feature_dim + LANES
    struct = jax.ShapeDtypeStruct

    inputs = (list_ids.T, spill_weight.T, list_pos.reshape(-1, LANES), vectors)
    send, seat = on_chip(
        lambda *refs: route_kernel(*refs, cap=cap, lists_here=lists_here),
        (struct((sent, width), BF16), struct((slot_count, row_count), jnp.int32)),
        *inputs,
        name="route",
        in_hbm=range(4),
        scratch=[
            *(pltpu.VMEM(a.shape, a.dtype) for a in inputs),
            pltpu.SemaphoreType.DMA((4,)),
        ],
    )
    got = lax.all_to_all(send.reshape(owners, half, width), "grp", 0, 0, tiled=True)
    got = got.reshape(sent, width)
    swap = [(0, 1), (1, 0)]
    peer = lax.ppermute(got, "rep", swap)
    chosen, rows = on_chip(
        own_shares_kernel,
        (struct((2 * sent, lists_here), BF16), struct((8, 2 * sent), F32)),
        got,
        old_centroids,
        name="own_shares",
    )
    peer_rows = lax.ppermute(rows, "rep", swap)
    sums, totals = on_chip(
        own_sums_kernel,
        (struct((lists_here, feature_dim), F32), struct((lists_here, LANES), F32)),
        got,
        rows,
        name="own_sums",
    )
    refined, owner_dist = on_chip(
        lambda *refs: refine_kernel(*refs, cap=cap),
        (struct((lists_here, feature_dim), F32), struct((owners, LANES), F32)),
        sums,
        totals,
        chosen,
        peer,
        peer_rows,
        got,
        old_centroids,
        name="refine",
        out_hbm=(0,),
        scratch=[
            pltpu.VMEM((lists_here, feature_dim), F32),
            pltpu.VMEM((2 * sent, LANES), F32),
            pltpu.SemaphoreType.DMA((BLOCKS,)),
        ],
    )
    seat_dist = lax.all_to_all(owner_dist.reshape(owners, 1, LANES), "grp", 0, 0, tiled=True)
    (new_dist,) = on_chip(
        lambda *refs: pick_kernel(*refs, cap=cap),
        (struct((slot_count, row_count), F32),),
        seat_dist.reshape(owners, LANES),
        seat,
        name="pick",
    )
    return refined, new_dist.T


def solution(mesh):
    return jax.shard_map(
        shards,
        mesh=mesh,
        in_specs=(
            P(("grp", "rep"), None),
            P(("grp", "rep"), None),
            P(("grp", "rep"), None),
            P(),
            P("grp", None),
        ),
        out_specs=(P("grp", None), P(("grp", "rep"), None)),
        check_vma=False,
    )
```

```python
import jax
import jax.numpy as jnp
from jax import lax
from jax.experimental import pallas as pl
from jax.experimental.pallas import tpu as pltpu
from jax.sharding import PartitionSpec as P

LANES = 128
CHUNK = 256
BLOCKS = 2
VMEM_LIMIT = 24 * 2**20
F32 = jnp.float32
BF16 = jnp.bfloat16


def iota(shape, dim):
    return lax.broadcasted_iota(jnp.int32, shape, dim)


def ones_where(mask):
    return jnp.where(mask, F32(1), F32(0)).astype(BF16)


def dot(a, b, contract=(1, 0)):
    return lax.dot_general(
        a, b, (((contract[0],), (contract[1],)), ((), ())), preferred_element_type=F32
    )


def pieces(value, count):
    result = []
    for _ in range(count):
        part = value.astype(BF16)
        result.append(part)
        value = value - part.astype(F32)
    return result


def dot_of_pieces(a, parts):
    return dot(jnp.concatenate([a] * len(parts), axis=1), jnp.concatenate(parts, axis=0))


def each(count, fn, axis):
    return jnp.concatenate([fn(k) for k in range(count)], axis=axis)


def route_kernel(
    ids_hbm, weight_hbm, table_hbm, vectors_hbm, send_ref, seat_ref, ids_ref, weight_ref, table_ref,
    vectors_ref, sems, *, cap, lists_here,
):
    copies = [
        pltpu.make_async_copy(source, target, sems.at[i])
        for i, (source, target) in enumerate(
            [(ids_hbm, ids_ref), (table_hbm, table_ref), (weight_hbm, weight_ref), (vectors_hbm, vectors_ref)]
        )
    ]
    for copy in copies:
        copy.start()
    slots, rows = ids_ref.shape
    feature_dim = vectors_ref.shape[1]
    half = cap // 2
    sent = send_ref.shape[0]
    owners = sent // half
    copies[0].wait()
    ids = ids_ref[...]
    live = ids >= 0
    safe = jnp.maximum(ids, 0)
    high, low = safe >> 7, safe & 127
    row_of_table = iota((table_ref.shape[0], rows), 0)
    picks = each(slots, lambda k: ones_where(row_of_table == high[k : k + 1]), 1)
    copies[1].wait()
    table = table_ref[...]
    digits = jnp.concatenate(
        [(table >> 8).astype(F32).astype(BF16), (table & 255).astype(F32).astype(BF16)], axis=1
    )
    found = dot(digits, picks, (0, 0))
    found = found[:LANES] * 256 + found[LANES:]
    lane_of_table = iota((LANES, rows), 0)
    place = each(
        slots,
        lambda k: jnp.sum(
            jnp.where(lane_of_table == low[k : k + 1], found[:, k * rows : (k + 1) * rows], 0.0),
            axis=0,
            keepdims=True,
        ),
        0,
    ).astype(jnp.int32)
    copies[2].wait()
    owner = jnp.where(live, place // lists_here, owners)
    code = (place % lists_here) * 8 + weight_ref[...]

    owner_iota = iota((owners, rows), 0)
    at_owner = [owner_iota == owner[k : k + 1] for k in range(slots)]
    before = ones_where(iota((rows, 2 * rows), 0) < iota((rows, 2 * rows), 1))
    counted = dot(each(slots, lambda k: ones_where(at_owner[k]), 0), before)
    carried = jnp.zeros((owners, rows), F32)
    ranks = []
    for k in range(slots):
        here = counted[k * owners : (k + 1) * owners]
        rank = jnp.where(at_owner[k], here[:, :rows] + carried, 0.0)
        ranks.append(jnp.sum(rank, axis=0, keepdims=True))
        carried = carried + here[:, rows:]
    rank = jnp.concatenate(ranks, axis=0).astype(jnp.int32)
    seat = jnp.where(live, (rank % 2) * sent + owner * half + rank // 2, -1)
    seat_ref[...] = seat

    copies[3].wait()
    vectors = vectors_ref[...]
    columns = send_ref.shape[1] - 2 * feature_dim
    spread = ones_where(iota((4 * rows, columns), 0) // rows == iota((4 * rows, columns), 1))
    for at in range(0, sent, rows):
        here = slice(at, at + rows)
        digits = []
        for b in range(2):
            seat_iota = iota((rows, rows), 0) + (b * sent + at)
            codes = jnp.zeros((rows, rows), jnp.int32)
            for k in range(slots):
                codes = jnp.where(seat_iota == seat[k : k + 1], code[k : k + 1], codes)
            digits += [(codes >> 6).astype(F32).astype(BF16), (codes & 63).astype(F32).astype(BF16)]
            send_ref[here, b * feature_dim : (b + 1) * feature_dim] = dot(
                ones_where(codes > 0), vectors
            ).astype(BF16)
        send_ref[here, 2 * feature_dim :] = dot(jnp.concatenate(digits, axis=1), spread).astype(BF16)


def seat_vectors(got_ref, feature_dim, chunk):
    return each(2, lambda b: got_ref[:, b * feature_dim + chunk.start : b * feature_dim + chunk.stop], 0)


def chunks_of(feature_dim):
    return [slice(at, at + CHUNK) for at in range(0, feature_dim, CHUNK)]


def folded(square):
    return sum(square[:, at : at + LANES] for at in range(0, square.shape[1], LANES))


def own_shares_kernel(got_ref, centroids_ref, chosen_ref, rows_ref):
    lists_here, feature_dim = centroids_ref.shape
    meta = got_ref[:, 2 * feature_dim :]
    columns = meta.astype(F32)
    code = each(
        2, lambda b: columns[:, 2 * b : 2 * b + 1] * 64 + columns[:, 2 * b + 1 : 2 * b + 2], 0
    ).astype(jnp.int32)
    seats = code.shape[0]
    for at in range(0, seats, LANES):
        here = slice(at, at + LANES)
        chosen_ref[here] = ones_where(iota((LANES, lists_here), 1) == (code[here] >> 3))
    to_rows = ones_where(iota((8, LANES), 0) == iota((8, LANES), 1))
    digits = dot(to_rows, meta, (1, 1))
    code_row = each(
        2, lambda b: digits[2 * b : 2 * b + 1] * 64 + digits[2 * b + 1 : 2 * b + 2], 1
    ).astype(jnp.int32)
    total = jnp.zeros((seats, LANES), F32)
    for chunk in chunks_of(feature_dim):
        centre = dot_of_pieces(chosen_ref[...], pieces(centroids_ref[:, chunk], 2))
        total = total + folded((seat_vectors(got_ref, feature_dim, chunk).astype(F32) - centre) ** 2)
    sq_norms = dot(jnp.ones((8, 3 * LANES), BF16), jnp.concatenate(pieces(total, 3), axis=1), (1, 1))
    shares = (code_row % 8).astype(F32) / (1.0 + sq_norms[0:1] / feature_dim)
    high, low = pieces(shares, 2)
    row = iota((8, seats), 0)
    rows_ref[...] = jnp.where(
        row == 0,
        high.astype(F32),
        jnp.where(row == 1, low.astype(F32), (code_row >> 3).astype(F32)),
    )


def placed(rows_ref, lists_here):
    rows = rows_ref[...]
    named = iota((lists_here, rows.shape[1]), 0) == rows[2:3].astype(jnp.int32)
    parts = [jnp.where(named, rows[i : i + 1], 0.0) for i in range(2)]
    totals = jnp.sum(parts[0] + parts[1], axis=1, keepdims=True)
    return jnp.concatenate([part.astype(BF16) for part in parts], axis=1), totals


def own_sums_kernel(got_ref, rows_ref, sums_ref, totals_ref):
    lists_here, feature_dim = sums_ref.shape
    parts, totals = placed(rows_ref, lists_here)
    totals_ref[...] = jnp.broadcast_to(totals, totals_ref.shape)
    for chunk in chunks_of(feature_dim):
        vectors = seat_vectors(got_ref, feature_dim, chunk)
        sums_ref[:, chunk] = dot(parts, jnp.concatenate([vectors] * 2, axis=0))


def refine_kernel(
    sums_ref, totals_ref, chosen_ref, peer_ref, peer_rows_ref, got_ref, centroids_ref, refined_hbm,
    dist_ref, refined_ref, seat_dist_ref, sems, *, cap,
):
    lists_here, feature_dim = centroids_ref.shape
    parts, peer_totals = placed(peer_rows_ref, lists_here)
    scale = 1.0 / (1.0 + (totals_ref[:, 0:1] + peer_totals))
    chunks = chunks_of(feature_dim)
    step = lists_here // BLOCKS
    copies = []
    for i in range(BLOCKS):
        here = slice(i * step, (i + 1) * step)
        for chunk in chunks:
            vectors = seat_vectors(peer_ref, feature_dim, chunk)
            sums = sums_ref[here, chunk] + dot(parts[here], jnp.concatenate([vectors] * 2, axis=0))
            refined_ref[here, chunk] = (centroids_ref[here, chunk] + sums) * scale[here]
        copies.append(
            pltpu.make_async_copy(refined_ref.at[here], refined_hbm.at[here], sems.at[i])
        )
        copies[-1].start()
    half = cap // 2
    sent = got_ref.shape[0]
    owners = sent // half
    total = jnp.zeros((2 * sent, LANES), F32)
    for chunk in chunks:
        centre = dot_of_pieces(chosen_ref[...], pieces(refined_ref[:, chunk], 2))
        total = total + folded((seat_vectors(got_ref, feature_dim, chunk).astype(F32) - centre) ** 2)
    dist = jnp.sum(total, axis=1, keepdims=True) / feature_dim
    seat_dist_ref[...] = jnp.broadcast_to(dist, seat_dist_ref.shape)
    lane = iota((owners, LANES), 1)
    by_owner = jnp.zeros((owners, LANES), F32)
    for a in range(half):
        for b in range(2):
            mine = seat_dist_ref[pl.ds(b * sent + a, owners, stride=half), :]
            by_owner = jnp.where(lane == 2 * a + b, mine, by_owner)
    dist_ref[...] = by_owner
    for copy in copies:
        copy.wait()


def pick_kernel(dist_ref, seat_ref, out_ref, *, cap):
    slots, rows = seat_ref.shape
    owners = dist_ref.shape[0]
    half = cap // 2
    sent = owners * half
    seat = seat_ref[...]
    owner = jnp.where(seat >= 0, (seat % sent) // half, owners)
    rank = (seat % half) * 2 + seat // sent
    by_rank = dist_ref[...].T[:8]
    owner_iota = iota((owners, rows), 0)
    at_owner = each(slots, lambda k: ones_where(owner_iota == owner[k : k + 1]), 1)
    found = dot(jnp.concatenate(pieces(by_rank, 3), axis=0), at_owner)
    found = found[:8] + found[8:16] + found[16:]
    rank_iota = iota((8, rows), 0)
    picked = each(
        slots,
        lambda k: jnp.sum(
            jnp.where(rank_iota == rank[k : k + 1], found[:, k * rows : (k + 1) * rows], 0.0),
            axis=0,
            keepdims=True,
        ),
        0,
    )
    out_ref[...] = jnp.where(seat >= 0, picked, 0.0)


def on_chip(kernel, outs, *args, name, in_hbm=(), out_hbm=(), scratch=()):
    def spec(i, away):
        return pl.BlockSpec(memory_space=pltpu.HBM if i in away else pltpu.VMEM)

    args = [
        pltpu.with_memory_space_constraint(a, pltpu.HBM) if i in in_hbm else a
        for i, a in enumerate(args)
    ]

    return pl.pallas_call(
        kernel,
        out_shape=outs,
        in_specs=[spec(i, in_hbm) for i in range(len(args))],
        out_specs=[spec(i, out_hbm) for i in range(len(outs))],
        scratch_shapes=list(scratch),
        compiler_params=pltpu.CompilerParams(vmem_limit_bytes=VMEM_LIMIT),
        name=name,
    )(*args)


def shards(vectors, list_ids, spill_weight, list_pos, old_centroids):
    owners = lax.axis_size("grp")
    row_count, slot_count = list_ids.shape
    lists_here, feature_dim = old_centroids.shape
    cap = row_count * slot_count // (2 * owners)
    half = cap // 2
    sent = owners * half
    width = 2 * feature_dim + LANES
    struct = jax.ShapeDtypeStruct

    inputs = (list_ids.T, spill_weight.T, list_pos.reshape(-1, LANES), vectors)
    send, seat = on_chip(
        lambda *refs: route_kernel(*refs, cap=cap, lists_here=lists_here),
        (struct((sent, width), BF16), struct((slot_count, row_count), jnp.int32)),
        *inputs,
        name="route",
        in_hbm=range(4),
        scratch=[
            *(pltpu.VMEM(a.shape, a.dtype) for a in inputs),
            pltpu.SemaphoreType.DMA((4,)),
        ],
    )
    got = lax.all_to_all(send.reshape(owners, half, width), "grp", 0, 0, tiled=True)
    got = got.reshape(sent, width)
    swap = [(0, 1), (1, 0)]
    peer = lax.ppermute(got, "rep", swap)
    chosen, rows = on_chip(
        own_shares_kernel,
        (struct((2 * sent, lists_here), BF16), struct((8, 2 * sent), F32)),
        got,
        old_centroids,
        name="own_shares",
    )
    peer_rows = lax.ppermute(rows, "rep", swap)
    sums, totals = on_chip(
        own_sums_kernel,
        (struct((lists_here, feature_dim), F32), struct((lists_here, LANES), F32)),
        got,
        rows,
        name="own_sums",
    )
    refined, owner_dist = on_chip(
        lambda *refs: refine_kernel(*refs, cap=cap),
        (struct((lists_here, feature_dim), F32), struct((owners, LANES), F32)),
        sums,
        totals,
        chosen,
        peer,
        peer_rows,
        got,
        old_centroids,
        name="refine",
        out_hbm=(0,),
        scratch=[
            pltpu.VMEM((lists_here, feature_dim), F32),
            pltpu.VMEM((2 * sent, LANES), F32),
            pltpu.SemaphoreType.DMA((BLOCKS,)),
        ],
    )
    seat_dist = lax.all_to_all(owner_dist.reshape(owners, 1, LANES), "grp", 0, 0, tiled=True)
    (new_dist,) = on_chip(
        lambda *refs: pick_kernel(*refs, cap=cap),
        (struct((slot_count, row_count), F32),),
        seat_dist.reshape(owners, LANES),
        seat,
        name="pick",
    )
    return refined, new_dist.T


def solution(mesh):
    return jax.shard_map(
        shards,
        mesh=mesh,
        in_specs=(
            P(("grp", "rep"), None),
            P(("grp", "rep"), None),
            P(("grp", "rep"), None),
            P(),
            P("grp", None),
        ),
        out_specs=(P("grp", None), P(("grp", "rep"), None)),
        check_vma=False,
    )
```

```python
import jax
import jax.numpy as jnp
from jax import lax
from jax.experimental import pallas as pl
from jax.experimental.pallas import tpu as pltpu
from jax.sharding import PartitionSpec as P

LANES = 128
CHUNK = 256
BLOCKS = 2
VMEM_LIMIT = 24 * 2**20
F32 = jnp.float32
BF16 = jnp.bfloat16


def iota(shape, dim):
    return lax.broadcasted_iota(jnp.int32, shape, dim)


def ones_where(mask):
    return jnp.where(mask, F32(1), F32(0)).astype(BF16)


def dot(a, b, contract=(1, 0)):
    return lax.dot_general(
        a, b, (((contract[0],), (contract[1],)), ((), ())), preferred_element_type=F32
    )


def pieces(value, count):
    result = []
    for _ in range(count):
        part = value.astype(BF16)
        result.append(part)
        value = value - part.astype(F32)
    return result


def dot_of_pieces(a, parts):
    return dot(jnp.concatenate([a] * len(parts), axis=1), jnp.concatenate(parts, axis=0))


def sum_of_parts(parts, b):
    both = dot(jnp.concatenate(parts, axis=0), b)
    return both[: parts[0].shape[0]] + both[parts[0].shape[0] :]


def each(count, fn, axis):
    return jnp.concatenate([fn(k) for k in range(count)], axis=axis)


def route_kernel(
    ids_hbm, weight_hbm, table_hbm, vectors_hbm, send_ref, seat_ref, ids_ref, weight_ref, table_ref,
    vectors_ref, sems, *, cap, lists_here,
):
    copies = [
        pltpu.make_async_copy(source, target, sems.at[i])
        for i, (source, target) in enumerate(
            [(ids_hbm, ids_ref), (table_hbm, table_ref), (weight_hbm, weight_ref), (vectors_hbm, vectors_ref)]
        )
    ]
    for copy in copies:
        copy.start()
    slots, rows = ids_ref.shape
    feature_dim = vectors_ref.shape[1]
    half = cap // 2
    sent = send_ref.shape[0]
    owners = sent // half
    copies[0].wait()
    ids = ids_ref[...]
    live = ids >= 0
    safe = jnp.maximum(ids, 0)
    high, low = safe >> 7, safe & 127
    row_of_table = iota((table_ref.shape[0], rows), 0)
    picks = each(slots, lambda k: ones_where(row_of_table == high[k : k + 1]), 1)
    copies[1].wait()
    table = table_ref[...]
    digits = jnp.concatenate(
        [(table >> 8).astype(F32).astype(BF16), (table & 255).astype(F32).astype(BF16)], axis=1
    )
    found = dot(digits, picks, (0, 0))
    found = found[:LANES] * 256 + found[LANES:]
    lane_of_table = iota((LANES, rows), 0)
    place = each(
        slots,
        lambda k: jnp.sum(
            jnp.where(lane_of_table == low[k : k + 1], found[:, k * rows : (k + 1) * rows], 0.0),
            axis=0,
            keepdims=True,
        ),
        0,
    ).astype(jnp.int32)
    copies[2].wait()
    owner = jnp.where(live, place // lists_here, owners)
    code = (place % lists_here) * 8 + weight_ref[...]

    owner_iota = iota((owners, rows), 0)
    at_owner = [owner_iota == owner[k : k + 1] for k in range(slots)]
    before = ones_where(iota((rows, 2 * rows), 0) < iota((rows, 2 * rows), 1))
    counted = dot(each(slots, lambda k: ones_where(at_owner[k]), 0), before)
    carried = jnp.zeros((owners, rows), F32)
    ranks = []
    for k in range(slots):
        here = counted[k * owners : (k + 1) * owners]
        rank = jnp.where(at_owner[k], here[:, :rows] + carried, 0.0)
        ranks.append(jnp.sum(rank, axis=0, keepdims=True))
        carried = carried + here[:, rows:]
    rank = jnp.concatenate(ranks, axis=0).astype(jnp.int32)
    seat = jnp.where(live, (rank % 2) * sent + owner * half + rank // 2, -1)
    seat_ref[...] = seat

    copies[3].wait()
    vectors = vectors_ref[...]
    columns = send_ref.shape[1] - 2 * feature_dim
    spread = ones_where(iota((4 * rows, columns), 0) // rows == iota((4 * rows, columns), 1))
    for at in range(0, sent, rows):
        here = slice(at, at + rows)
        digits = []
        for b in range(2):
            seat_iota = iota((rows, rows), 0) + (b * sent + at)
            codes = jnp.zeros((rows, rows), jnp.int32)
            for k in range(slots):
                codes = jnp.where(seat_iota == seat[k : k + 1], code[k : k + 1], codes)
            digits += [(codes >> 6).astype(F32).astype(BF16), (codes & 63).astype(F32).astype(BF16)]
            send_ref[here, b * feature_dim : (b + 1) * feature_dim] = dot(
                ones_where(codes > 0), vectors
            ).astype(BF16)
        send_ref[here, 2 * feature_dim :] = dot(jnp.concatenate(digits, axis=1), spread).astype(BF16)


def seat_vectors(got_ref, feature_dim, chunk):
    return each(2, lambda b: got_ref[:, b * feature_dim + chunk.start : b * feature_dim + chunk.stop], 0)


def chunks_of(feature_dim):
    return [slice(at, at + CHUNK) for at in range(0, feature_dim, CHUNK)]


def folded(square):
    return sum(square[:, at : at + LANES] for at in range(0, square.shape[1], LANES))


def own_shares_kernel(got_ref, centroids_ref, chosen_ref, rows_ref):
    lists_here, feature_dim = centroids_ref.shape
    meta = got_ref[:, 2 * feature_dim :]
    columns = meta.astype(F32)
    code = each(
        2, lambda b: columns[:, 2 * b : 2 * b + 1] * 64 + columns[:, 2 * b + 1 : 2 * b + 2], 0
    ).astype(jnp.int32)
    seats = code.shape[0]
    for at in range(0, seats, LANES):
        here = slice(at, at + LANES)
        chosen_ref[here] = ones_where(iota((LANES, lists_here), 1) == (code[here] >> 3))
    to_rows = ones_where(iota((8, LANES), 0) == iota((8, LANES), 1))
    digits = dot(to_rows, meta, (1, 1))
    code_row = each(
        2, lambda b: digits[2 * b : 2 * b + 1] * 64 + digits[2 * b + 1 : 2 * b + 2], 1
    ).astype(jnp.int32)
    total = jnp.zeros((seats, LANES), F32)
    for chunk in chunks_of(feature_dim):
        centre = dot_of_pieces(chosen_ref[...], pieces(centroids_ref[:, chunk], 2))
        total = total + folded((seat_vectors(got_ref, feature_dim, chunk).astype(F32) - centre) ** 2)
    sq_norms = dot(jnp.ones((8, 3 * LANES), BF16), jnp.concatenate(pieces(total, 3), axis=1), (1, 1))
    shares = (code_row % 8).astype(F32) / (1.0 + sq_norms[0:1] / feature_dim)
    high, low = pieces(shares, 2)
    row = iota((8, seats), 0)
    rows_ref[...] = jnp.where(
        row == 0,
        high.astype(F32),
        jnp.where(row == 1, low.astype(F32), (code_row >> 3).astype(F32)),
    )


def placed(rows_ref, lists_here):
    rows = rows_ref[...]
    named = iota((lists_here, rows.shape[1]), 0) == rows[2:3].astype(jnp.int32)
    parts = [jnp.where(named, rows[i : i + 1], 0.0) for i in range(2)]
    totals = jnp.sum(parts[0] + parts[1], axis=1, keepdims=True)
    return [part.astype(BF16) for part in parts], totals


def own_sums_kernel(got_ref, rows_ref, sums_ref, totals_ref):
    lists_here, feature_dim = sums_ref.shape
    parts, totals = placed(rows_ref, lists_here)
    totals_ref[...] = jnp.broadcast_to(totals, totals_ref.shape)
    for chunk in chunks_of(feature_dim):
        vectors = seat_vectors(got_ref, feature_dim, chunk)
        sums_ref[:, chunk] = sum_of_parts(parts, vectors)


def refine_kernel(
    sums_ref, totals_ref, chosen_ref, peer_ref, peer_rows_ref, got_ref, centroids_ref, refined_hbm,
    dist_ref, refined_ref, seat_dist_ref, sems, *, cap,
):
    lists_here, feature_dim = centroids_ref.shape
    parts, peer_totals = placed(peer_rows_ref, lists_here)
    scale = 1.0 / (1.0 + (totals_ref[:, 0:1] + peer_totals))
    chunks = chunks_of(feature_dim)
    step = lists_here // BLOCKS
    copies = []
    for i in range(BLOCKS):
        here = slice(i * step, (i + 1) * step)
        for chunk in chunks:
            vectors = seat_vectors(peer_ref, feature_dim, chunk)
            sums = sums_ref[here, chunk] + sum_of_parts([part[here] for part in parts], vectors)
            refined_ref[here, chunk] = (centroids_ref[here, chunk] + sums) * scale[here]
        copies.append(
            pltpu.make_async_copy(refined_ref.at[here], refined_hbm.at[here], sems.at[i])
        )
        copies[-1].start()
    half = cap // 2
    sent = got_ref.shape[0]
    owners = sent // half
    total = jnp.zeros((2 * sent, LANES), F32)
    for chunk in chunks:
        centre = dot_of_pieces(chosen_ref[...], pieces(refined_ref[:, chunk], 2))
        total = total + folded((seat_vectors(got_ref, feature_dim, chunk).astype(F32) - centre) ** 2)
    dist = jnp.sum(total, axis=1, keepdims=True) / feature_dim
    seat_dist_ref[...] = jnp.broadcast_to(dist, seat_dist_ref.shape)
    lane = iota((owners, LANES), 1)
    by_owner = jnp.zeros((owners, LANES), F32)
    for a in range(half):
        for b in range(2):
            mine = seat_dist_ref[pl.ds(b * sent + a, owners, stride=half), :]
            by_owner = jnp.where(lane == 2 * a + b, mine, by_owner)
    dist_ref[...] = by_owner
    for copy in copies:
        copy.wait()


def pick_kernel(dist_ref, seat_ref, out_ref, *, cap):
    slots, rows = seat_ref.shape
    owners = dist_ref.shape[0]
    half = cap // 2
    sent = owners * half
    seat = seat_ref[...]
    owner = jnp.where(seat >= 0, (seat % sent) // half, owners)
    rank = (seat % half) * 2 + seat // sent
    by_rank = dist_ref[...].T[:8]
    owner_iota = iota((owners, rows), 0)
    at_owner = each(slots, lambda k: ones_where(owner_iota == owner[k : k + 1]), 1)
    found = dot(jnp.concatenate(pieces(by_rank, 3), axis=0), at_owner)
    found = found[:8] + found[8:16] + found[16:]
    rank_iota = iota((8, rows), 0)
    picked = each(
        slots,
        lambda k: jnp.sum(
            jnp.where(rank_iota == rank[k : k + 1], found[:, k * rows : (k + 1) * rows], 0.0),
            axis=0,
            keepdims=True,
        ),
        0,
    )
    out_ref[...] = jnp.where(seat >= 0, picked, 0.0)


def on_chip(kernel, outs, *args, name, in_hbm=(), out_hbm=(), scratch=()):
    def spec(i, away):
        return pl.BlockSpec(memory_space=pltpu.HBM if i in away else pltpu.VMEM)

    args = [
        pltpu.with_memory_space_constraint(a, pltpu.HBM) if i in in_hbm else a
        for i, a in enumerate(args)
    ]

    return pl.pallas_call(
        kernel,
        out_shape=outs,
        in_specs=[spec(i, in_hbm) for i in range(len(args))],
        out_specs=[spec(i, out_hbm) for i in range(len(outs))],
        scratch_shapes=list(scratch),
        compiler_params=pltpu.CompilerParams(vmem_limit_bytes=VMEM_LIMIT),
        name=name,
    )(*args)


def shards(vectors, list_ids, spill_weight, list_pos, old_centroids):
    owners = lax.axis_size("grp")
    row_count, slot_count = list_ids.shape
    lists_here, feature_dim = old_centroids.shape
    cap = row_count * slot_count // (2 * owners)
    half = cap // 2
    sent = owners * half
    width = 2 * feature_dim + LANES
    struct = jax.ShapeDtypeStruct

    inputs = (list_ids.T, spill_weight.T, list_pos.reshape(-1, LANES), vectors)
    send, seat = on_chip(
        lambda *refs: route_kernel(*refs, cap=cap, lists_here=lists_here),
        (struct((sent, width), BF16), struct((slot_count, row_count), jnp.int32)),
        *inputs,
        name="route",
        in_hbm=range(4),
        scratch=[
            *(pltpu.VMEM(a.shape, a.dtype) for a in inputs),
            pltpu.SemaphoreType.DMA((4,)),
        ],
    )
    got = lax.all_to_all(send.reshape(owners, half, width), "grp", 0, 0, tiled=True)
    got = got.reshape(sent, width)
    swap = [(0, 1), (1, 0)]
    peer = lax.ppermute(got, "rep", swap)
    chosen, rows = on_chip(
        own_shares_kernel,
        (struct((2 * sent, lists_here), BF16), struct((8, 2 * sent), F32)),
        got,
        old_centroids,
        name="own_shares",
    )
    peer_rows = lax.ppermute(rows, "rep", swap)
    sums, totals = on_chip(
        own_sums_kernel,
        (struct((lists_here, feature_dim), F32), struct((lists_here, LANES), F32)),
        got,
        rows,
        name="own_sums",
    )
    refined, owner_dist = on_chip(
        lambda *refs: refine_kernel(*refs, cap=cap),
        (struct((lists_here, feature_dim), F32), struct((owners, LANES), F32)),
        sums,
        totals,
        chosen,
        peer,
        peer_rows,
        got,
        old_centroids,
        name="refine",
        out_hbm=(0,),
        scratch=[
            pltpu.VMEM((lists_here, feature_dim), F32),
            pltpu.VMEM((2 * sent, LANES), F32),
            pltpu.SemaphoreType.DMA((BLOCKS,)),
        ],
    )
    seat_dist = lax.all_to_all(owner_dist.reshape(owners, 1, LANES), "grp", 0, 0, tiled=True)
    (new_dist,) = on_chip(
        lambda *refs: pick_kernel(*refs, cap=cap),
        (struct((slot_count, row_count), F32),),
        seat_dist.reshape(owners, LANES),
        seat,
        name="pick",
    )
    return refined, new_dist.T


def solution(mesh):
    return jax.shard_map(
        shards,
        mesh=mesh,
        in_specs=(
            P(("grp", "rep"), None),
            P(("grp", "rep"), None),
            P(("grp", "rep"), None),
            P(),
            P("grp", None),
        ),
        out_specs=(P("grp", None), P(("grp", "rep"), None)),
        check_vma=False,
    )
```
